32 devices in a mesh: groups: 2 (over y), row: 4 (over x, core), col: 4 (over z).
Axes of the slice: x: 2, y: 2, z: 4, core: 2. Of those that a mesh axis runs over, the one named last changes fastest.
Arguments:
- single: bfloat16 [512, 768], P(('groups', 'row'), 'col'), parts along dimension 0, may hold values from -16 to 16
- pair: bfloat16 [512, 256, 128], P(('groups', 'row'), 'col'), parts along dimension 0, may hold values from -6 to 6
- chain: int32 [512], P('groups'), parts along dimension 0, may hold values from 0 to 7, never falling along the last dimension, each value on 1 to 64 neighbouring positions
- live: int32 [512], P('groups'), parts along dimension 0, may hold values 0 or 1
- step_index: int32 [2], P('groups'), parts along dimension 0, may hold values from 0 to 999
- time_scale: bfloat16 [256, 768], P(None, 'col'), may hold values from -0.375 to 0.375
- time_shift: bfloat16 [256, 768], P(None, 'col'), may hold values from -0.375 to 0.375
- w_query: bfloat16 [768, 768], P(None, 'col'), may hold values from -0.21875 to 0.21875
- w_key: bfloat16 [768, 768], P(None, 'col'), may hold values from -0.21875 to 0.21875
- w_value: bfloat16 [768, 768], P(None, 'col'), may hold values from -0.21875 to 0.21875
- w_gate: bfloat16 [768, 768], P(None, 'col'), may hold values from -0.21875 to 0.21875
- w_out: bfloat16 [768, 768], P(None, 'col'), may hold values from -0.21875 to 0.21875
- pair_gain: float32 [128], replicated, may hold values from 0.1 to 1.9
- bias_weight: bfloat16 [128, 12], replicated, may hold values from -30 to 30
- chain_bias: float32 [2, 12], replicated, may hold values from -4 to 4
- outer_gain: float32 [768], P('col'), may hold values from 0.1 to 1.9
- w_left: float32 [768, 32], P('col'), may hold values from -0.21875 to 0.21875
- w_right: float32 [768, 32], P('col'), may hold values from -0.21875 to 0.21875
- w_outer: bfloat16 [32, 32, 128], replicated, may hold values from -0.1875 to 0.1875
- outer_bias: float32 [128], replicated, may hold values from -4 to 4
- trans_gain: float32 [128], replicated, may hold values from 0.1 to 1.9
- w_in: bfloat16 [128, 1024], replicated, may hold values from -0.5 to 0.5
- w_down: bfloat16 [512, 128], replicated, may hold values from -0.25 to 0.25
Outputs:
- single_out: bfloat16 [512, 768], P(('groups', 'row'), 'col'), parts along dimension 0
- pair_out: bfloat16 [512, 256, 128], P(('groups', 'row'), 'col'), parts along dimension 0
The draws below stay inside these ranges and needn't reach their ends.
There are 2 independent parts, one for each index of `groups`. The reference program is written for one: setup_inputs(seed, part) draws one part's arguments, and reference() takes and returns one part's arrays. A program takes and returns all parts, laid end to end along the dimension named above; an argument that names none is the same for every part. Nothing has to cross between parts.
Inputs may be any that keep to these rules, and one draw needn't show every extreme that they name: chain numbers never fall along the residues.
All inputs are finite; a program needn't handle non-finite values.
Results may differ from the reference program's by a relative error of at most 0.0095.
Values may be sent and summed in bfloat16 or wider, within the bound.
No kernel may reach another device: no remote copies, remote signals or barrier semaphores. Data moves between devices by JAX's collectives and lax.ppermute only.
A program may use at most 64 MiB of HBM per device.

```python
import math
import jax
import jax.numpy as jnp
import numpy as np
from jax import lax

RB = 64
CS = 768
HEADS = 12
HD = 64
CZ = 128
HID = 512
OPM = 32
TFREQ = 256
TSTEPS = 1000
CHAINS = 8
RES = 256


def draw_single(key, part):
    key_base, key_rough = jax.random.split(jax.random.fold_in(key, 11), 2)
    base = jax.random.normal(key_base, (RES, CS), jnp.float32)
    ramp = jnp.exp(jnp.linspace(jnp.log(0.5), jnp.log(2.0), CS))
    rough = jax.random.uniform(key_rough, (CS,), jnp.float32, 0.6, 1.6)
    values = base * ramp * rough
    return jnp.clip(values, -16.0, 16.0).astype(jnp.bfloat16)


def draw_bias_weight(key, part):
    key_base = jax.random.fold_in(jax.random.fold_in(key, 23), 0)
    values = jnp.clip(jax.random.normal(key_base, (CZ, HEADS), jnp.float32), -4.0, 4.0) / jnp.sqrt(CZ * 1.0)
    return jnp.clip(values, -30.0, 30.0).astype(jnp.bfloat16)


def with_ends(entries, stream_key, low, top_value):
    longest = entries.shape.index(max(entries.shape))
    spots = []
    for shift in (0, 1):
        where = [jax.random.randint(jax.random.fold_in(stream_key, axis), (), 0, length) for axis, length in enumerate(entries.shape)]
        where[longest] = (where[longest] + shift) % entries.shape[longest]
        spots.append(tuple(where))
    return entries.at[spots[0]].set(low).at[spots[1]].set(top_value)


def steps_of(stream_key, extent, shards, low, largest):
    def one(dim, shards_of):
        heights = jax.random.uniform(jax.random.fold_in(jax.random.fold_in(stream_key, 6), dim), (shards_of,), jnp.float32, low / len(shards), largest / len(shards))
        return jnp.repeat(jnp.exp(heights), extent[dim] // shards_of).reshape((-1,) + (1,) * (len(extent) - dim - 1))

    level = one(*shards[0])
    for cut in shards[1:]:
        level = level * one(*cut)
    return level


def profile(number_of, total, reach, lean):
    portions = [(1 << 20) // math.isqrt(rank ** lean) + 1 for rank in range(2, number_of + 1)]
    spare, holding = total - reach - (number_of - 1), [1] * (number_of - 1)
    while spare > 0:
        candidates = [i for i in range(number_of - 1) if holding[i] < reach]
        whole, remaining = sum([portions[i] for i in candidates]), spare
        for i in candidates:
            more = min(reach - holding[i], max(1, remaining * portions[i] // whole), spare)
            holding[i] = holding[i] + more
            spare = spare - more
    return np.array([reach] + holding)


def uneven_parts(key, amount, total, most, skew):
    if amount == 2:
        one = jax.random.randint(key, (), max(1, total - most), min(most, total - 1) + 1)
        return jnp.stack([one, total - one])
    tallies = jnp.asarray(profile(amount, total, most, skew), jnp.int32)
    couples = (amount - 1) // 2
    donor, taker = tallies[1:1 + 2 * couples:2], tallies[2:2 + 2 * couples:2]
    room = jnp.minimum(donor - 1, most - taker)
    passed = jax.random.randint(jax.random.fold_in(key, 1), (couples,), 0, 1 << 20) % (room + 1)
    tallies = tallies.at[1:1 + 2 * couples:2].set(donor - passed).at[2:2 + 2 * couples:2].set(taker + passed)
    return tallies[jax.random.permutation(jax.random.fold_in(key, 2), amount)]


def bell_draw(stream_key, shape, width, limit, shards=(), held_as=jnp.bfloat16):
    values = width * jax.random.normal(stream_key, shape, jnp.float32)
    if shards:
        values = values * steps_of(stream_key, shape, shards, -0.22, 0.18)
    return jnp.clip(values, -limit, limit).astype(held_as)


def setup_inputs(seed: int = 0, part: int = 0) -> dict:
    keys = jax.random.split(jax.random.key(seed), 24)
    part_keys = jax.random.split(jax.random.fold_in(keys[23], part), 24)
    single = draw_single(jax.random.fold_in(jax.random.fold_in(keys[23], part), 71), part)
    pair = bell_draw(part_keys[1], (RES, RES, CZ), 1.0, 6.0, ((0, 4), (1, 4)))
    chain = jnp.searchsorted(jnp.cumsum(uneven_parts(part_keys[2], CHAINS, RES, RES // 4, 1)), jnp.arange(RES), side="right").astype(jnp.int32)
    live = with_ends((jax.random.randint(part_keys[3], (RES,), 0, 8) < 7).astype(jnp.int32), jax.random.fold_in(part_keys[3], 1), 0, 1)
    step_index = jax.random.randint(part_keys[4], (1,), 0, TSTEPS).astype(jnp.int32)
    time_scale = bell_draw(keys[5], (TFREQ, CS), TFREQ ** -0.5, 0.375, ((1, 4),))
    time_shift = bell_draw(keys[6], (TFREQ, CS), TFREQ ** -0.5, 0.375, ((1, 4),))
    w_query = bell_draw(keys[7], (CS, CS), CS ** -0.5, 0.21875, ((1, 4),))
    w_key = bell_draw(keys[8], (CS, CS), CS ** -0.5, 0.21875, ((1, 4),))
    w_value = bell_draw(keys[9], (CS, CS), CS ** -0.5, 0.21875, ((1, 4),))
    w_gate = bell_draw(keys[10], (CS, CS), CS ** -0.5, 0.21875, ((1, 4),))
    w_out = bell_draw(keys[11], (CS, CS), CS ** -0.5, 0.21875, ((1, 4),))
    pair_gain = jnp.clip(1.0 + 0.18 * jax.random.normal(keys[12], (CZ,), jnp.float32), 0.1, 1.9)
    bias_weight = draw_bias_weight(jax.random.fold_in(keys[23], 71), part)
    chain_bias = bell_draw(keys[14], (2, HEADS), 1.0, 4.0, (), jnp.float32)
    outer_gain = jnp.clip(1.0 + 0.18 * jax.random.normal(keys[15], (CS,), jnp.float32), 0.1, 1.9)
    w_left = bell_draw(keys[16], (CS, OPM), CS ** -0.5, 0.21875, ((0, 4),), jnp.float32)
    w_right = bell_draw(keys[17], (CS, OPM), CS ** -0.5, 0.21875, ((0, 4),), jnp.float32)
    w_outer = bell_draw(keys[18], (OPM, OPM, CZ), (OPM * OPM) ** -0.5, 0.1875)
    outer_bias = bell_draw(keys[19], (CZ,), 1.0, 4.0, (), jnp.float32)
    trans_gain = jnp.clip(1.0 + 0.18 * jax.random.normal(keys[20], (CZ,), jnp.float32), 0.1, 1.9)
    w_in = bell_draw(keys[21], (CZ, 2 * HID), CZ ** -0.5, 0.5)
    w_down = bell_draw(keys[22], (HID, CZ), HID ** -0.5, 0.25)
    return {"single": single, "pair": pair, "chain": chain, "live": live, "step_index": step_index, "time_scale": time_scale, "time_shift": time_shift, "w_query": w_query, "w_key": w_key, "w_value": w_value, "w_gate": w_gate, "w_out": w_out, "pair_gain": pair_gain, "bias_weight": bias_weight, "chain_bias": chain_bias, "outer_gain": outer_gain, "w_left": w_left, "w_right": w_right, "w_outer": w_outer, "outer_bias": outer_bias, "trans_gain": trans_gain, "w_in": w_in, "w_down": w_down}


EPSILON = 1e-05
MASKED = -1000000000.0

def channel_norm(values, gain):
    row_mean = lax.optimization_barrier(jnp.mean(values, axis=-1, keepdims=True))
    spread = lax.optimization_barrier(jnp.mean(values * values, axis=-1, keepdims=True)) - row_mean * row_mean
    return (values - row_mean) * lax.rsqrt(spread + EPSILON) * gain

def time_embed(step_index, count):
    halfway = count // 2
    ladder = jnp.arange(halfway).astype(jnp.float32)
    freqs = jnp.exp(-math.log(10000.0) * ladder / halfway)
    angles = step_index[0].astype(jnp.float32) * freqs
    return jnp.concatenate([jnp.sin(angles), jnp.cos(angles)])

def head_scores(query_rows, key_rows, bias_terms, head_count):
    query_heads = query_rows.reshape(query_rows.shape[0], head_count, -1)
    key_heads = key_rows.reshape(key_rows.shape[0], head_count, -1)
    raw = jnp.einsum('qhd,khd->hqk', query_heads.astype(jnp.float32), key_heads.astype(jnp.float32))
    return raw * query_heads.shape[2] ** (-0.5) + bias_terms

def transition(updated, gain, w_in, w_down):
    flat = updated.reshape(-1, updated.shape[-1])
    normed = channel_norm(flat, gain).astype(jnp.bfloat16)
    mixed = jnp.dot(normed, w_in, preferred_element_type=jnp.float32)
    halfway = w_down.shape[0]
    hidden = (jax.nn.silu(mixed[:, :halfway]) * mixed[:, halfway:]).astype(jnp.bfloat16)
    result = flat + jnp.dot(hidden, w_down, preferred_element_type=jnp.float32)
    return result.astype(jnp.bfloat16).reshape(updated.shape)

def reference(single, pair, chain, live, step_index, time_scale, time_shift, w_query, w_key, w_value, w_gate, w_out, pair_gain, bias_weight, chain_bias, outer_gain, w_left, w_right, w_outer, outer_bias, trans_gain, w_in, w_down):
    single_f = single.astype(jnp.float32)
    embedded = time_embed(step_index, TFREQ).astype(jnp.bfloat16)
    mod_scale = jnp.dot(embedded[None], time_scale, preferred_element_type=jnp.float32)[0]
    mod_shift = jnp.dot(embedded[None], time_shift, preferred_element_type=jnp.float32)[0]
    normed = (channel_norm(single_f, 1.0 + mod_scale) + mod_shift).astype(jnp.bfloat16)
    query_all = jnp.dot(normed, w_query, preferred_element_type=jnp.float32).astype(jnp.bfloat16)
    key_all = jnp.dot(normed, w_key, preferred_element_type=jnp.float32).astype(jnp.bfloat16)
    value_all = jnp.dot(normed, w_value, preferred_element_type=jnp.float32).astype(jnp.bfloat16)
    gate_all = jnp.dot(normed, w_gate, preferred_element_type=jnp.float32).astype(jnp.bfloat16)
    value_heads = value_all.reshape(RES, HEADS, HD).astype(jnp.float32)
    live_key = jnp.where(live == 1, 0.0, MASKED).astype(jnp.float32)
    blocks = jnp.arange(RES // RB).astype(jnp.int32)

    def attend(block_id):
        row_start = (block_id * RB).astype(jnp.int32)
        pair_rows = lax.dynamic_slice_in_dim(pair, row_start, RB, 0)
        pair_normed = channel_norm(pair_rows.astype(jnp.float32), pair_gain).astype(jnp.bfloat16)
        bias_terms = jnp.einsum('qkc,ch->hqk', pair_normed.astype(jnp.float32), bias_weight.astype(jnp.float32))
        chain_rows = lax.dynamic_slice_in_dim(chain, row_start, RB, 0)
        same_chain = chain_rows[:, None] == chain[None, :]
        chain_terms = jnp.where(same_chain[None], chain_bias[0][:, None, None], chain_bias[1][:, None, None])
        bias_terms = bias_terms + chain_terms + live_key[None, None, :]
        query_rows = lax.dynamic_slice_in_dim(query_all, row_start, RB, 0)
        scores = head_scores(query_rows, key_all, bias_terms, HEADS)
        row_top = lax.optimization_barrier(jnp.max(scores, axis=2))
        weights_exp = jnp.exp(scores - row_top[:, :, None])
        row_sum = lax.optimization_barrier(jnp.sum(weights_exp, axis=2))
        attended = jnp.einsum('hqk,khd->qhd', weights_exp, value_heads, precision=lax.Precision.HIGHEST)
        attended = (attended / row_sum.T[:, :, None]).reshape(RB, CS)
        gate_rows = lax.dynamic_slice_in_dim(gate_all, row_start, RB, 0)
        return (jax.nn.sigmoid(gate_rows.astype(jnp.float32)) * attended).astype(jnp.bfloat16)
    gated = lax.map(attend, blocks).reshape(RES, CS)
    single_out = (single_f + jnp.dot(gated, w_out, preferred_element_type=jnp.float32)).astype(jnp.bfloat16)
    outer_normed = channel_norm(single_out.astype(jnp.float32), outer_gain)
    left = jnp.dot(outer_normed, w_left, precision=lax.Precision.HIGHEST).astype(jnp.bfloat16)
    right = jnp.dot(outer_normed, w_right, precision=lax.Precision.HIGHEST).astype(jnp.bfloat16)
    left_mix = jnp.einsum('ip,pqc->iqc', left.astype(jnp.float32), w_outer.astype(jnp.float32), precision=lax.Precision.HIGHEST)
    right_f = right.astype(jnp.float32)
    live_f = live.astype(jnp.float32)

    def update(block_id):
        row_start = (block_id * RB).astype(jnp.int32)
        pair_rows = lax.dynamic_slice_in_dim(pair, row_start, RB, 0)
        left_rows = lax.dynamic_slice_in_dim(left_mix, row_start, RB, 0)
        live_rows = lax.dynamic_slice_in_dim(live_f, row_start, RB, 0)
        outer = jnp.einsum('iqc,jq->ijc', left_rows, right_f, precision=lax.Precision.HIGHEST) + outer_bias
        outer = outer * (live_rows[:, None] * live_f[None, :])[:, :, None]
        updated = pair_rows.astype(jnp.float32) + outer
        return transition(updated, trans_gain, w_in, w_down)
    pair_out = lax.map(update, blocks).reshape(RES, RES, CZ)
    return (single_out, pair_out)
```

```python
import math

import jax
import jax.numpy as jnp
from jax import lax
from jax.experimental import pallas as pl
from jax.experimental.pallas import tpu as pltpu
from jax.sharding import PartitionSpec as P

EPSILON = 1e-05
MASKED = -1000000000.0
FULL_GRANT = 67043328
AUX_CHAIN = 0
AUX_LIVE = 32
AUX_VECTORS = 40
AUX_BIAS = 48
AUX_KEYS = 56
AUX_QUERIES = 120
AUX_WEIGHT = 184
AUX_ROWS = 200


def broadcast(array, axis, root):
    mine = lax.axis_index(axis) == root
    return lax.psum(jnp.where(mine, array, jnp.zeros_like(array)), axis)


def channel_norm(values, gain):
    row_mean = jnp.mean(values, axis=-1, keepdims=True)
    spread = jnp.mean(values * values, axis=-1, keepdims=True) - row_mean * row_mean
    return (values - row_mean) * lax.rsqrt(spread + EPSILON) * gain


def time_embed(step_index, count):
    halfway = count // 2
    ladder = jnp.arange(halfway).astype(jnp.float32)
    freqs = jnp.exp(-math.log(10000.0) * ladder / halfway)
    angles = step_index[0].astype(jnp.float32) * freqs
    return jnp.concatenate([jnp.sin(angles), jnp.cos(angles)])


def head_scores(query_rows, key_rows, bias_terms, head_count):
    query_heads = query_rows.reshape(query_rows.shape[0], head_count, -1)
    key_heads = key_rows.reshape(key_rows.shape[0], head_count, -1)
    raw = jnp.einsum("qhd,khd->hqk", query_heads, key_heads, preferred_element_type=jnp.float32)
    return raw * query_heads.shape[2] ** (-0.5) + bias_terms


def weighted_values(weights_exp, value_rows, head_count):
    value_heads = value_rows.reshape(value_rows.shape[0], head_count, -1).astype(jnp.float32)
    summed = jnp.einsum("hqk,khd->qhd", weights_exp, value_heads, precision=lax.Precision.HIGHEST)
    return summed.reshape(summed.shape[0], -1)


def divide_heads(summed, totals):
    row_count = summed.shape[0]
    head_count = totals.shape[0]
    return (summed.reshape(row_count, head_count, -1) / totals.T[:, :, None]).reshape(row_count, -1)


def transition(flat, gain, w_in, w_down):
    normed = channel_norm(flat, gain).astype(jnp.bfloat16)
    mixed = jnp.dot(normed, w_in, preferred_element_type=jnp.float32)
    halfway = w_down.shape[0]
    hidden = (jax.nn.silu(mixed[:, :halfway]) * mixed[:, halfway:]).astype(jnp.bfloat16)
    return (flat + jnp.dot(hidden, w_down, preferred_element_type=jnp.float32)).astype(jnp.bfloat16)


def body(
    single,
    pair,
    chain,
    live,
    step_index,
    time_scale,
    time_shift,
    w_query,
    w_key,
    w_value,
    w_gate,
    w_out,
    pair_gain,
    bias_weight,
    chain_bias,
    outer_gain,
    w_left,
    w_right,
    w_outer,
    outer_bias,
    trans_gain,
    w_in,
    w_down,
):
    block_rows = single.shape[0]
    model_width = w_query.shape[0]
    head_count = chain_bias.shape[1]
    row_place = lax.axis_index("row")
    col_place = lax.axis_index("col")
    query_start = row_place * block_rows
    key_start = col_place * block_rows
    chain_query = lax.dynamic_slice_in_dim(chain, query_start, block_rows, 0)
    chain_key = lax.dynamic_slice_in_dim(chain, key_start, block_rows, 0)
    live_query = lax.dynamic_slice_in_dim(live, query_start, block_rows, 0).astype(jnp.float32)
    live_keys = lax.dynamic_slice_in_dim(live, key_start, block_rows, 0)
    single_f = single.astype(jnp.float32)
    totals = lax.psum((jnp.sum(single_f, axis=1), jnp.sum(single_f * single_f, axis=1)), "col")
    row_mean = totals[0] / model_width
    inv_std = lax.rsqrt(totals[1] / model_width - row_mean * row_mean + EPSILON)
    embedded = time_embed(step_index, time_scale.shape[0]).astype(jnp.bfloat16)
    mod_scale = jnp.dot(embedded[None], time_scale, preferred_element_type=jnp.float32)[0]
    mod_shift = jnp.dot(embedded[None], time_shift, preferred_element_type=jnp.float32)[0]
    normed = (
        (single_f - row_mean[:, None]) * inv_std[:, None] * (1.0 + mod_scale) + mod_shift
    ).astype(jnp.bfloat16)
    normed_full = lax.all_gather(normed, "col", axis=1, tiled=True)
    query_part = jnp.dot(normed_full, w_query, preferred_element_type=jnp.float32).astype(
        jnp.bfloat16
    )
    key_part = jnp.dot(normed_full, w_key, preferred_element_type=jnp.float32).astype(jnp.bfloat16)
    value_part = jnp.dot(normed_full, w_value, preferred_element_type=jnp.float32).astype(
        jnp.bfloat16
    )
    gate_part = jnp.dot(normed_full, w_gate, preferred_element_type=jnp.float32).astype(
        jnp.bfloat16
    )
    query_full, key_full, value_full, gate_full = (
        lax.all_gather(query_part, "col", axis=1, tiled=True),
        lax.all_gather(key_part, "col", axis=1, tiled=True),
        lax.all_gather(value_part, "col", axis=1, tiled=True),
        lax.all_gather(gate_part, "col", axis=1, tiled=True),
    )
    key_cols, value_cols = (
        broadcast(key_full, "row", col_place),
        broadcast(value_full, "row", col_place),
    )
    pair_normed = channel_norm(pair.astype(jnp.float32), pair_gain).astype(jnp.bfloat16)
    bias_terms = jnp.einsum(
        "qkc,ch->hqk", pair_normed, bias_weight, preferred_element_type=jnp.float32
    )
    same_chain = chain_query[:, None] == chain_key[None, :]
    chain_terms = jnp.where(
        same_chain[None], chain_bias[0][:, None, None], chain_bias[1][:, None, None]
    )
    live_terms = jnp.where(live_keys == 1, 0.0, MASKED).astype(jnp.float32)
    bias_terms = bias_terms + chain_terms + live_terms[None, None, :]
    scores = head_scores(query_full, key_cols, bias_terms, head_count)
    row_top = lax.pmax(jnp.max(scores, axis=2), "col")
    weights_exp = jnp.exp(scores - row_top[:, :, None])
    row_sum, summed = lax.psum(
        (jnp.sum(weights_exp, axis=2), weighted_values(weights_exp, value_cols, head_count)), "col"
    )
    attended = divide_heads(summed, row_sum)
    gated = (jax.nn.sigmoid(gate_full.astype(jnp.float32)) * attended).astype(jnp.bfloat16)
    single_out = (single_f + jnp.dot(gated, w_out, preferred_element_type=jnp.float32)).astype(
        jnp.bfloat16
    )
    updated_single = single_out.astype(jnp.float32)
    gained = updated_single * outer_gain
    joint = lax.psum(
        (
            jnp.sum(updated_single, axis=1),
            jnp.sum(updated_single * updated_single, axis=1),
            jnp.dot(gained, w_left, precision=lax.Precision.HIGHEST),
            jnp.dot(gained, w_right, precision=lax.Precision.HIGHEST),
            jnp.dot(outer_gain[None], w_left, precision=lax.Precision.HIGHEST)[0],
            jnp.dot(outer_gain[None], w_right, precision=lax.Precision.HIGHEST)[0],
        ),
        "col",
    )
    out_mean = joint[0] / model_width
    out_inv = lax.rsqrt(joint[1] / model_width - out_mean * out_mean + EPSILON)
    left_full = out_inv[:, None] * (joint[2] - out_mean[:, None] * joint[4][None, :])
    right_full = out_inv[:, None] * (joint[3] - out_mean[:, None] * joint[5][None, :])
    left_rows = left_full.astype(jnp.bfloat16)
    right_rows = right_full.astype(jnp.bfloat16)
    right_cols = broadcast(right_rows, "row", col_place)
    left_mix = jnp.einsum("ip,pqc->iqc", left_rows, w_outer, preferred_element_type=jnp.float32)
    outer = (
        jnp.einsum(
            "iqc,jq->ijc", left_mix, right_cols.astype(jnp.float32), precision=lax.Precision.HIGHEST
        )
        + outer_bias
    )
    outer = outer * (live_query[:, None] * live_keys.astype(jnp.float32)[None, :])[:, :, None]
    updated = pair.astype(jnp.float32) + outer
    flat = updated.reshape(-1, updated.shape[-1])
    total_rows = flat.shape[0]
    piece_rows = math.gcd(total_rows, 1024)
    pieces = flat.reshape(total_rows // piece_rows, piece_rows, flat.shape[1])
    pair_out = lax.map(lambda piece: transition(piece, trans_gain, w_in, w_down), pieces).reshape(
        pair.shape
    )
    return (single_out, pair_out)


def dot_f32(a, b, contract=((1,), (0,))):
    return lax.dot_general(a, b, (contract, ((), ())), preferred_element_type=jnp.float32)


def dot_exact(a, b, contract=((1,), (0,))):
    return lax.dot_general(
        a, b, (contract, ((), ())), precision=lax.Precision.HIGHEST, preferred_element_type=jnp.float32
    )


def split_pair(values):
    high = values.astype(jnp.bfloat16)
    return high, (values - high.astype(jnp.float32)).astype(jnp.bfloat16)


def fetch(pairs, semaphores):
    copies = [
        pltpu.make_async_copy(source, target, semaphores.at[n])
        for n, (source, target) in enumerate(pairs)
    ]
    for copy in copies:
        copy.start()
    return copies


def window(row, start, lanes):
    return pltpu.roll(row, (row.shape[1] - start) % row.shape[1], 1)[:, :lanes]


def as_column(row):
    size = row.shape[1]
    shape = (size, size)
    on_diagonal = lax.broadcasted_iota(jnp.int32, shape, 0) == lax.broadcasted_iota(
        jnp.int32, shape, 1
    )
    spread = jnp.where(on_diagonal, jnp.broadcast_to(row, shape), 0.0)
    return jnp.sum(spread, axis=1, keepdims=True)


def pack_kernel(
    step_hbm,
    scale_hbm,
    shift_hbm,
    gain_hbm,
    left_hbm,
    right_hbm,
    chain_hbm,
    live_hbm,
    weight_hbm,
    chain_bias_hbm,
    outer_bias_hbm,
    trans_gain_hbm,
    pair_gain_hbm,
    single_hbm,
    packed_hbm,
    aux_hbm,
    out_ref,
    aux_ref,
    step_ref,
    scale_ref,
    shift_ref,
    gain_ref,
    left_ref,
    right_ref,
    chain_ref,
    live_ref,
    weight_ref,
    chain_bias_ref,
    outer_bias_ref,
    trans_gain_ref,
    pair_gain_ref,
    semaphores,
    out_semaphores,
):
    rows, width = single_hbm.shape
    keys, channels = rows, aux_ref.shape[1]
    half = rows // 2
    copies = fetch(
        (
            (step_hbm, step_ref),
            (scale_hbm, scale_ref),
            (shift_hbm, shift_ref),
            (gain_hbm, gain_ref),
            (left_hbm, left_ref),
            (right_hbm, right_ref),
            (chain_hbm, chain_ref),
            (live_hbm, live_ref),
            (weight_hbm, weight_ref),
            (chain_bias_hbm, chain_bias_ref),
            (outer_bias_hbm, outer_bias_ref),
            (trans_gain_hbm, trans_gain_ref),
            (pair_gain_hbm, pair_gain_ref),
            (single_hbm, out_ref.at[pl.ds(0, rows), :]),
        ),
        semaphores,
    )
    for copy in copies:
        copy.wait()
    halfway = scale_ref.shape[1] // 2
    ladder = lax.broadcasted_iota(jnp.int32, (16, halfway), 1).astype(jnp.float32)
    freqs = jnp.exp(-math.log(10000.0) * ladder / halfway)
    angles = step_ref[0].astype(jnp.float32) * freqs
    embedded = jnp.concatenate([jnp.sin(angles), jnp.cos(angles)], axis=1).astype(jnp.bfloat16)
    contract = ((1,), (1,))
    mod_scale = dot_f32(embedded, scale_ref[...], contract)[:1]
    mod_shift = dot_f32(embedded, shift_ref[...], contract)[:1]
    gain = jnp.broadcast_to(gain_ref[...], (8, width))
    factors = jnp.concatenate([left_ref[...], right_ref[...]], axis=0)
    factor_sum = dot_exact(gain, factors, contract)[:1]
    filler = jnp.zeros((1, width - factors.shape[0]), jnp.float32)
    sums = jnp.concatenate([factor_sum, filler], axis=1)
    tail = []
    for row in (mod_scale, mod_shift, sums):
        high = row.astype(jnp.bfloat16).astype(jnp.float32)
        tail += [high, row - high]
    tail.append(jnp.zeros((out_ref.shape[0] - rows - len(tail), width), jnp.float32))
    out_ref[rows:, :] = jnp.concatenate(tail, axis=0).astype(jnp.bfloat16)
    packed_store = pltpu.make_async_copy(out_ref, packed_hbm, out_semaphores.at[0])
    packed_store.start()

    chain = chain_ref[...].astype(jnp.float32)
    live = live_ref[...].astype(jnp.float32)
    query_start, key_start = lax.axis_index("row") * rows, lax.axis_index("col") * keys
    chain_column = as_column(window(chain, query_start, rows))
    chain_row = window(chain, key_start, keys)
    distance = jnp.concatenate(
        [chain_column[:half] - chain_row, chain_column[half:] - chain_row], axis=1
    )
    live_keys = window(live, key_start, keys)
    live_terms = jnp.where(live_keys == 1.0, 0.0, MASKED)
    aux_ref[AUX_CHAIN : AUX_CHAIN + half, :] = distance
    aux_ref[AUX_LIVE : AUX_LIVE + 1, :] = jnp.concatenate([live_terms, live_terms], axis=1)
    aux_ref[AUX_VECTORS : AUX_VECTORS + 1, :] = outer_bias_ref[...]
    aux_ref[AUX_VECTORS + 1 : AUX_VECTORS + 2, :] = trans_gain_ref[...]
    aux_ref[AUX_VECTORS + 2 : AUX_VECTORS + 3, :] = pair_gain_ref[...]
    head_count = weight_ref.shape[0]
    aux_ref[AUX_BIAS : AUX_BIAS + 2, :head_count] = chain_bias_ref[...]
    aux_ref[AUX_WEIGHT : AUX_WEIGHT + head_count, :] = weight_ref[...].astype(jnp.float32)
    aux_ref[AUX_KEYS : AUX_KEYS + keys, :] = jnp.broadcast_to(as_column(live_keys), (keys, channels))
    live_queries = as_column(window(live, query_start, rows))
    aux_ref[AUX_QUERIES : AUX_QUERIES + rows, :] = jnp.broadcast_to(live_queries, (rows, channels))
    aux_store = pltpu.make_async_copy(aux_ref, aux_hbm, out_semaphores.at[1])
    aux_store.start()
    packed_store.wait()
    aux_store.wait()


def bias_kernel(aux_ref, pair_ref, out_ref):
    half = out_ref.shape[2]
    keys, channels = pair_ref.shape[1:]
    heads_here = out_ref.shape[1]
    head_count = out_ref.shape[0] * heads_here
    step = 8
    live_terms = aux_ref[AUX_LIVE : AUX_LIVE + 1, :]
    gain = aux_ref[AUX_VECTORS + 2 : AUX_VECTORS + 3, :]
    weight = aux_ref[AUX_WEIGHT : AUX_WEIGHT + 16, :].astype(jnp.bfloat16)
    same_bias = [aux_ref[AUX_BIAS : AUX_BIAS + 1, h : h + 1] for h in range(head_count)]
    other_bias = [aux_ref[AUX_BIAS + 1 : AUX_BIAS + 2, h : h + 1] for h in range(head_count)]
    for start in range(0, half, step):
        parts = []
        for base in (start, half + start):
            block = pair_ref[base : base + step].astype(jnp.float32).reshape(step * keys, channels)
            parts.append(channel_norm(block, gain).astype(jnp.bfloat16))
        normed = []
        for k in range(step):
            normed.append(parts[0][k * keys : (k + 1) * keys])
            normed.append(parts[1][k * keys : (k + 1) * keys])
        terms = dot_f32(weight, jnp.concatenate(normed, axis=0), ((1,), (1,)))
        terms = terms.reshape(terms.shape[0], step, 2 * keys)
        same = aux_ref[AUX_CHAIN + start : AUX_CHAIN + start + step, :] == 0.0
        for head in range(head_count):
            chain_terms = jnp.where(same, same_bias[head], other_bias[head])
            out_ref[head // heads_here, head % heads_here, start : start + step, :] = (
                terms[head] + chain_terms
            ) + live_terms


def project_kernel(*refs):
    count = len(refs) - 8
    blocks = refs[:count]
    query_w, key_w, value_w, gate_w, query_out, kv_out, gate_out, ordered = refs[count:]
    rows, width = query_out.shape
    model_width = query_w.shape[1]
    values = [block[:rows, :].astype(jnp.float32) for block in blocks]
    total = sum(jnp.sum(v, axis=1, keepdims=True) for v in values)
    squares = sum(jnp.sum(v * v, axis=1, keepdims=True) for v in values)
    row_mean = total / model_width
    inv_std = lax.rsqrt(squares / model_width - row_mean * row_mean + EPSILON)
    for k, (block, v) in enumerate(zip(blocks, values)):
        tail = block[rows : rows + 8, :].astype(jnp.float32)
        scale = tail[0:1] + tail[1:2]
        shift = tail[2:3] + tail[3:4]
        normed = (v - row_mean) * inv_std * (1.0 + scale) + shift
        ordered[lax.axis_index("col") ^ k] = normed.astype(jnp.bfloat16)
    normed = jnp.concatenate([ordered[b] for b in range(count)], axis=1)
    contract = ((1,), (1,))
    query_out[...] = dot_f32(normed, query_w[...], contract).astype(jnp.bfloat16)
    kv_out[:, :width] = dot_f32(normed, key_w[...], contract).astype(jnp.bfloat16)
    kv_out[:, width:] = dot_f32(normed, value_w[...], contract).astype(jnp.bfloat16)
    gate_out[...] = dot_f32(normed, gate_w[...], contract).astype(jnp.bfloat16)


def attend_kernel(query_ref, gate_ref, *refs):
    count = (len(refs) - 3) // 2
    kvs = refs[:count]
    biases = refs[count : 2 * count]
    out_ref, kv_all, bias_all = refs[2 * count :]
    rows, width = query_ref.shape
    heads_here = biases[0].shape[0]
    head_size = width // heads_here
    half = rows // 2
    for k in range(count):
        kv_all[pl.ds(pl.multiple_of((lax.axis_index("row") ^ k) * rows, rows), rows), :] = kvs[k][...]
        bias_all[lax.axis_index("col") ^ k] = biases[k][...]
    for head in range(heads_here):
        lanes = slice(head * head_size, (head + 1) * head_size)
        value_lanes = slice(width + head * head_size, width + (head + 1) * head_size)
        raw = dot_f32(query_ref[:, lanes], kv_all[:, lanes], ((1,), (1,)))
        tops = [bias_all[b, head][:, :rows] for b in range(count)]
        lows = [bias_all[b, head][:, rows:] for b in range(count)]
        bias = jnp.concatenate(
            [jnp.concatenate(tops, axis=1), jnp.concatenate(lows, axis=1)], axis=0
        )
        scores = raw * head_size ** (-0.5) + bias
        weights = jnp.exp(scores - jnp.max(scores, axis=1, keepdims=True))
        total = jnp.sum(weights, axis=1, keepdims=True)
        high, low = split_pair(weights)
        values = kv_all[:, value_lanes]
        attended = (dot_f32(high, values) + dot_f32(low, values)) / total
        gate = jax.nn.sigmoid(gate_ref[:, lanes].astype(jnp.float32))
        out_ref[:, lanes] = (gate * attended).astype(jnp.bfloat16)


def output_kernel(single_ref, gain_ref, out_w, left_w, right_w, *refs):
    blocks = refs[:-3]
    single_out, message, ordered = refs[-3:]
    rows, width = single_ref.shape
    half = rows // 2
    for k, block in enumerate(blocks):
        ordered[lax.axis_index("col") ^ k] = block[...]
    gated = jnp.concatenate([ordered[b] for b in range(len(blocks))], axis=1)
    contract = ((1,), (1,))
    total = dot_f32(gated, out_w[...], contract)
    result = (single_ref[...].astype(jnp.float32) + total).astype(jnp.bfloat16)
    single_out[...] = result
    values = result.astype(jnp.float32)
    block_mean = jnp.sum(values, axis=1, keepdims=True) / width
    centered = values - block_mean
    block_var = jnp.sum(centered * centered, axis=1, keepdims=True) / width
    gain_high, gain_low = split_pair(centered * gain_ref[...])
    factor_high, factor_low = split_pair(jnp.concatenate([left_w[...], right_w[...]], axis=0))
    partial = (
        dot_f32(gain_high, factor_high, contract)
        + dot_f32(gain_low, factor_high, contract)
        + dot_f32(gain_high, factor_low, contract)
    )
    lane = lax.broadcasted_iota(jnp.int32, (rows, 128), 1)
    stats = jnp.where(lane == 0, block_mean, jnp.where(lane == 1, block_var, 0.0))
    stats = jnp.transpose(stats)[:8]
    high = stats.astype(jnp.bfloat16).astype(jnp.float32)
    stats = jnp.concatenate([high, stats - high], axis=1).astype(jnp.bfloat16)
    packed = jnp.concatenate([partial[:half], partial[half:]], axis=1).astype(jnp.bfloat16)
    for slot in range(message.shape[0]):
        message[slot, :half, :] = packed
        message[slot, half:, :] = stats


def factor_rows(parts, sums, model_width, factors, which):
    half = parts[0].shape[0] - 8
    lanes = slice(which * factors, (which + 1) * factors)
    far_lanes = slice((which + 2) * factors, (which + 3) * factors)
    means, variances, partials, colsums = [], [], [], []
    for part, tail in zip(parts, sums):
        values = part.astype(jnp.float32)
        stats = values[half:, : 2 * half] + values[half:, 2 * half :]
        means.append(stats[0:1])
        variances.append(stats[1:2])
        partials.append(
            jnp.concatenate([values[:half, lanes], values[:half, far_lanes]], axis=0)
        )
        colsums.append(tail[:, lanes])
    count = len(parts)
    mean = sum(means) / count
    spread = sum(v + (m - mean) * (m - mean) for v, m in zip(variances, means)) / count
    inv_std = as_column(lax.rsqrt(spread + EPSILON))
    shifts = [as_column(m - mean) for m in means]
    total = sum(p + m * s for p, m, s in zip(partials, shifts, colsums))
    return (inv_std * total).astype(jnp.bfloat16)


def update_kernel(
    single_ref,
    message_ref,
    pair_ref,
    aux_ref,
    outer_w_ref,
    w_in_ref,
    w_down_ref,
    *refs,
):
    blocks = refs[:-8]
    single_hbm, out_hbm, out_ref, mix_ref, right_ref, gate_w_ref, semaphore, semaphores = refs[-8:]
    rows, keys, channels = pair_ref.shape
    count = len(blocks)
    factors = outer_w_ref.shape[0]
    halfway = w_down_ref.shape[0]
    steps = semaphores.shape[0]
    step_rows = rows // steps
    single_copy = pltpu.make_async_copy(single_ref, single_hbm, semaphore)
    single_copy.start()

    sums = []
    for block in blocks:
        tail = block[rows : rows + 8, :].astype(jnp.float32)
        sums.append(tail[4:5] + tail[5:6])
    model_width = blocks[0].shape[1] * count
    lefts = [message_ref[lax.axis_index("row") * count + (lax.axis_index("col") ^ k)] for k in range(count)]
    rights = [message_ref[lax.axis_index("col") * count + (lax.axis_index("col") ^ k)] for k in range(count)]
    left = factor_rows(lefts, sums, model_width, factors, 0)
    right = factor_rows(rights, sums, model_width, factors, 1)
    live_keys = aux_ref[AUX_KEYS : AUX_KEYS + keys, :]
    live_queries = aux_ref[AUX_QUERIES : AUX_QUERIES + rows, :]
    spare = right_ref.shape[1] - 2 * factors
    live_right = live_keys[:, :factors].astype(jnp.bfloat16)
    right = right * live_right
    right_ref[...] = jnp.concatenate([right, right, live_right[:, :spare]], axis=1)
    left = left * live_queries[:, :factors].astype(jnp.bfloat16)
    mix = dot_f32(left, outer_w_ref[...]).reshape(rows, factors, channels)
    high, low = split_pair(mix)
    mix_ref[:, :factors, :] = high
    mix_ref[:, factors : 2 * factors, :] = low
    bias = aux_ref[AUX_VECTORS : AUX_VECTORS + 1, :]
    bias_high = bias.astype(jnp.bfloat16).astype(jnp.float32)
    pick = lax.broadcasted_iota(jnp.int32, (spare, channels), 0)
    bias_rows = jnp.where(pick == 0, bias_high, jnp.where(pick == 1, bias - bias_high, 0.0))
    mix_ref[:, 2 * factors :, :] = (live_queries[:, None, :] * bias_rows[None]).astype(jnp.bfloat16)
    gate_w_ref[...] = w_in_ref[:, :halfway] * jnp.asarray(0.5, w_in_ref.dtype)

    def copy_out(step):
        block = pl.ds(step * step_rows, step_rows)
        return pltpu.make_async_copy(out_ref.at[block], out_hbm.at[block], semaphores.at[step])

    def advance(step, carry):
        start = step * step_rows
        mixes = [mix_ref[start + i] for i in range(step_rows)]
        outers = dot_f32(right_ref[...], jnp.concatenate(mixes, axis=1))
        pieces = []
        for i in range(step_rows):
            outer = outers[:, i * channels : (i + 1) * channels]
            pieces.append(pair_ref[start + i].astype(jnp.float32) + outer)
        flat = jnp.concatenate(pieces, axis=0)
        normed = channel_norm(flat, aux_ref[AUX_VECTORS + 1 : AUX_VECTORS + 2, :]).astype(jnp.bfloat16)
        gate = dot_f32(normed, gate_w_ref[...])
        up = dot_f32(normed, w_in_ref[:, halfway:])
        hidden = ((gate + gate * jnp.tanh(gate)) * up).astype(jnp.bfloat16)
        result = flat + dot_f32(hidden, w_down_ref[...])
        out_ref[pl.ds(start, step_rows)] = result.astype(jnp.bfloat16).reshape(
            step_rows, keys, channels
        )
        copy_out(step).start()
        return carry

    lax.fori_loop(0, steps, advance, 0)
    for step in range(steps):
        copy_out(step).wait()
    single_copy.wait()


def local_call(
    kernel, operands, outs, name, scratch=(), hbm=(), hbm_out=False, grant=24 * 2**20, flops=0
):
    def spec(n):
        space = pltpu.HBM if n in hbm else pltpu.VMEM
        return pl.BlockSpec(memory_space=space)

    out_space = pltpu.HBM if hbm_out else pltpu.VMEM
    out_specs = [pl.BlockSpec(memory_space=out_space) for _ in outs]
    if len(outs) == 1:
        outs, out_specs = outs[0], out_specs[0]
    return pl.pallas_call(
        kernel,
        out_shape=outs,
        in_specs=[spec(n) for n in range(len(operands))],
        out_specs=out_specs,
        scratch_shapes=list(scratch),
        compiler_params=pltpu.CompilerParams(vmem_limit_bytes=grant),
        cost_estimate=pl.CostEstimate(flops=flops, bytes_accessed=2**18, transcendentals=0),
        name=name,
    )(*operands)


def exchange(array, axis, count):
    return [
        lax.ppermute(array, axis, [(i, i ^ k) for i in range(count)]) for k in range(1, count)
    ]


def headwise_body(
    single,
    pair,
    chain,
    live,
    step_index,
    time_scale,
    time_shift,
    w_query,
    w_key,
    w_value,
    w_gate,
    w_out,
    pair_gain,
    bias_weight,
    chain_bias,
    outer_gain,
    w_left,
    w_right,
    w_outer,
    outer_bias,
    trans_gain,
    w_in,
    w_down,
):
    bf16, f32 = jnp.bfloat16, jnp.float32
    rows, width = single.shape
    keys, channels = pair.shape[1:]
    half = rows // 2
    head_count = chain_bias.shape[1]
    count = lax.axis_size("col")
    heads_here = head_count // count
    factors = w_left.shape[1]
    col_place = lax.axis_index("col")
    shape = jax.ShapeDtypeStruct
    packed, aux = local_call(
        pack_kernel,
        (
            step_index,
            time_scale.T,
            time_shift.T,
            outer_gain[None],
            w_left.T,
            w_right.T,
            chain[None],
            live[None],
            bias_weight.T,
            chain_bias,
            outer_bias[None],
            trans_gain[None],
            pair_gain[None],
            single,
        ),
        [
            shape((rows + 16, width), bf16),
            shape((AUX_ROWS, channels), f32),
        ],
        "pack",
        scratch=(
            pltpu.VMEM((rows + 16, width), bf16),
            pltpu.VMEM((AUX_ROWS, channels), f32),
            pltpu.SMEM((1,), jnp.int32),
            pltpu.VMEM((width, time_scale.shape[0]), bf16),
            pltpu.VMEM((width, time_scale.shape[0]), bf16),
            pltpu.VMEM((1, width), f32),
            pltpu.VMEM((factors, width), f32),
            pltpu.VMEM((factors, width), f32),
            pltpu.VMEM((1, chain.shape[0]), jnp.int32),
            pltpu.VMEM((1, live.shape[0]), jnp.int32),
            pltpu.VMEM(bias_weight.T.shape, bf16),
            pltpu.VMEM(chain_bias.shape, f32),
            pltpu.VMEM((1, channels), f32),
            pltpu.VMEM((1, channels), f32),
            pltpu.VMEM((1, channels), f32),
            pltpu.SemaphoreType.DMA((14,)),
            pltpu.SemaphoreType.DMA((2,)),
        ),
        hbm=tuple(range(14)),
        hbm_out=True,
        grant=FULL_GRANT,
        flops=10**6,
    )
    blocks = [packed] + exchange(packed, "col", count)

    bias = local_call(
        bias_kernel,
        (aux, pair),
        [shape((count, heads_here, half, 2 * keys), f32)],
        "pair_bias",
        flops=10**10,
    )
    biases = [lax.dynamic_index_in_dim(bias, col_place, 0, keepdims=False)]
    for k in range(1, count):
        piece = lax.dynamic_index_in_dim(bias, col_place ^ k, 0, keepdims=False)
        biases.append(lax.ppermute(piece, "col", [(i, i ^ k) for i in range(count)]))

    query, kv, gate = local_call(
        project_kernel,
        (*blocks, w_query.T, w_key.T, w_value.T, w_gate.T),
        [shape((rows, width), bf16), shape((rows, 2 * width), bf16), shape((rows, width), bf16)],
        "project",
        scratch=(pltpu.VMEM((count, rows, width), bf16),),
        flops=10**8,
    )
    kvs = [kv] + exchange(kv, "row", count)
    gated = local_call(
        attend_kernel,
        (query, gate, *kvs, *biases),
        [shape((rows, width), bf16)],
        "attend",
        scratch=(
            pltpu.VMEM((count * rows, 2 * width), bf16),
            pltpu.VMEM((count, heads_here, half, 2 * keys), f32),
        ),
        flops=10**8,
    )
    gateds = [gated] + exchange(gated, "col", count)
    result, message = local_call(
        output_kernel,
        (single, outer_gain[None], w_out.T, w_left.T, w_right.T, *gateds),
        [shape((rows, width), bf16), shape((count * count, half + 8, 2 * keys), bf16)],
        "project_out",
        scratch=(pltpu.VMEM((count, rows, width), bf16),),
        flops=10**7,
    )
    outer_flat = w_outer.reshape(factors, factors * channels)
    message, outer_flat = lax.optimization_barrier((message, outer_flat))
    message = lax.all_to_all(message, ("row", "col"), 0, 0)

    steps = 8
    single_out, pair_out = local_call(
        update_kernel,
        (
            result,
            message,
            pair,
            aux,
            outer_flat,
            w_in,
            w_down,
            *blocks,
        ),
        [shape((rows, width), bf16), shape(pair.shape, bf16)],
        "pair_update",
        scratch=(
            pltpu.VMEM(pair.shape, bf16),
            pltpu.VMEM((rows, 2 * factors + 16, channels), bf16),
            pltpu.VMEM((keys, 2 * factors + 16), bf16),
            pltpu.VMEM((w_in.shape[0], w_down.shape[0]), bf16),
            pltpu.SemaphoreType.DMA,
            pltpu.SemaphoreType.DMA((steps,)),
        ),
        hbm_out=True,
        flops=2 * 10**9,
    )
    return (single_out, pair_out)


def pick_body(mesh):
    rows, cols = mesh.shape["row"], mesh.shape["col"]

    def chosen(*arrays):
        single, pair, chain_bias = arrays[0], arrays[1], arrays[14]
        fits = (
            rows == cols
            and cols & (cols - 1) == 0
            and chain_bias.shape[1] % cols == 0
            and single.shape[0] == pair.shape[1] == 64
            and 4 * arrays[16].shape[1] == pair.shape[2]
            and chain_bias.shape[1] <= AUX_ROWS - AUX_WEIGHT
            and pair.shape[2] == 128
        )
        return headwise_body(*arrays) if fits else body(*arrays)

    return chosen


def solution(mesh):
    in_specs = (
        P(("groups", "row"), "col"),
        P(("groups", "row"), "col", None),
        P("groups"),
        P("groups"),
        P("groups"),
        P(None, "col"),
        P(None, "col"),
        P(None, "col"),
        P(None, "col"),
        P(None, "col"),
        P(None, "col"),
        P(None, "col"),
        P(),
        P(),
        P(),
        P("col"),
        P("col", None),
        P("col", None),
        P(),
        P(),
        P(),
        P(),
        P(),
    )
    out_specs = (P(("groups", "row"), "col"), P(("groups", "row"), "col", None))
    return jax.shard_map(
        pick_body(mesh), mesh=mesh, in_specs=in_specs, out_specs=out_specs, check_vma=False)
```

```python
import math

import jax
import jax.numpy as jnp
from jax import lax
from jax.experimental import pallas as pl
from jax.experimental.pallas import tpu as pltpu
from jax.sharding import PartitionSpec as P

EPSILON = 1e-05
MASKED = -1000000000.0
AUX_CHAIN = 0
AUX_LIVE = 32
AUX_VECTORS = 40
AUX_BIAS = 48
AUX_KEYS = 56
AUX_QUERIES = 120
AUX_WEIGHT = 184
AUX_ROWS = 200


def broadcast(array, axis, root):
    mine = lax.axis_index(axis) == root
    return lax.psum(jnp.where(mine, array, jnp.zeros_like(array)), axis)


def channel_norm(values, gain):
    row_mean = jnp.mean(values, axis=-1, keepdims=True)
    spread = jnp.mean(values * values, axis=-1, keepdims=True) - row_mean * row_mean
    return (values - row_mean) * lax.rsqrt(spread + EPSILON) * gain


def time_embed(step_index, count):
    halfway = count // 2
    ladder = jnp.arange(halfway).astype(jnp.float32)
    freqs = jnp.exp(-math.log(10000.0) * ladder / halfway)
    angles = step_index[0].astype(jnp.float32) * freqs
    return jnp.concatenate([jnp.sin(angles), jnp.cos(angles)])


def head_scores(query_rows, key_rows, bias_terms, head_count):
    query_heads = query_rows.reshape(query_rows.shape[0], head_count, -1)
    key_heads = key_rows.reshape(key_rows.shape[0], head_count, -1)
    raw = jnp.einsum("qhd,khd->hqk", query_heads, key_heads, preferred_element_type=jnp.float32)
    return raw * query_heads.shape[2] ** (-0.5) + bias_terms


def weighted_values(weights_exp, value_rows, head_count):
    value_heads = value_rows.reshape(value_rows.shape[0], head_count, -1).astype(jnp.float32)
    summed = jnp.einsum("hqk,khd->qhd", weights_exp, value_heads, precision=lax.Precision.HIGHEST)
    return summed.reshape(summed.shape[0], -1)


def divide_heads(summed, totals):
    row_count = summed.shape[0]
    head_count = totals.shape[0]
    return (summed.reshape(row_count, head_count, -1) / totals.T[:, :, None]).reshape(row_count, -1)


def transition(flat, gain, w_in, w_down):
    normed = channel_norm(flat, gain).astype(jnp.bfloat16)
    mixed = jnp.dot(normed, w_in, preferred_element_type=jnp.float32)
    halfway = w_down.shape[0]
    hidden = (jax.nn.silu(mixed[:, :halfway]) * mixed[:, halfway:]).astype(jnp.bfloat16)
    return (flat + jnp.dot(hidden, w_down, preferred_element_type=jnp.float32)).astype(jnp.bfloat16)


def body(
    single,
    pair,
    chain,
    live,
    step_index,
    time_scale,
    time_shift,
    w_query,
    w_key,
    w_value,
    w_gate,
    w_out,
    pair_gain,
    bias_weight,
    chain_bias,
    outer_gain,
    w_left,
    w_right,
    w_outer,
    outer_bias,
    trans_gain,
    w_in,
    w_down,
):
    block_rows = single.shape[0]
    model_width = w_query.shape[0]
    head_count = chain_bias.shape[1]
    row_place = lax.axis_index("row")
    col_place = lax.axis_index("col")
    query_start = row_place * block_rows
    key_start = col_place * block_rows
    chain_query = lax.dynamic_slice_in_dim(chain, query_start, block_rows, 0)
    chain_key = lax.dynamic_slice_in_dim(chain, key_start, block_rows, 0)
    live_query = lax.dynamic_slice_in_dim(live, query_start, block_rows, 0).astype(jnp.float32)
    live_keys = lax.dynamic_slice_in_dim(live, key_start, block_rows, 0)
    single_f = single.astype(jnp.float32)
    totals = lax.psum((jnp.sum(single_f, axis=1), jnp.sum(single_f * single_f, axis=1)), "col")
    row_mean = totals[0] / model_width
    inv_std = lax.rsqrt(totals[1] / model_width - row_mean * row_mean + EPSILON)
    embedded = time_embed(step_index, time_scale.shape[0]).astype(jnp.bfloat16)
    mod_scale = jnp.dot(embedded[None], time_scale, preferred_element_type=jnp.float32)[0]
    mod_shift = jnp.dot(embedded[None], time_shift, preferred_element_type=jnp.float32)[0]
    normed = (
        (single_f - row_mean[:, None]) * inv_std[:, None] * (1.0 + mod_scale) + mod_shift
    ).astype(jnp.bfloat16)
    normed_full = lax.all_gather(normed, "col", axis=1, tiled=True)
    query_part = jnp.dot(normed_full, w_query, preferred_element_type=jnp.float32).astype(
        jnp.bfloat16
    )
    key_part = jnp.dot(normed_full, w_key, preferred_element_type=jnp.float32).astype(jnp.bfloat16)
    value_part = jnp.dot(normed_full, w_value, preferred_element_type=jnp.float32).astype(
        jnp.bfloat16
    )
    gate_part = jnp.dot(normed_full, w_gate, preferred_element_type=jnp.float32).astype(
        jnp.bfloat16
    )
    query_full, key_full, value_full, gate_full = (
        lax.all_gather(query_part, "col", axis=1, tiled=True),
        lax.all_gather(key_part, "col", axis=1, tiled=True),
        lax.all_gather(value_part, "col", axis=1, tiled=True),
        lax.all_gather(gate_part, "col", axis=1, tiled=True),
    )
    key_cols, value_cols = (
        broadcast(key_full, "row", col_place),
        broadcast(value_full, "row", col_place),
    )
    pair_normed = channel_norm(pair.astype(jnp.float32), pair_gain).astype(jnp.bfloat16)
    bias_terms = jnp.einsum(
        "qkc,ch->hqk", pair_normed, bias_weight, preferred_element_type=jnp.float32
    )
    same_chain = chain_query[:, None] == chain_key[None, :]
    chain_terms = jnp.where(
        same_chain[None], chain_bias[0][:, None, None], chain_bias[1][:, None, None]
    )
    live_terms = jnp.where(live_keys == 1, 0.0, MASKED).astype(jnp.float32)
    bias_terms = bias_terms + chain_terms + live_terms[None, None, :]
    scores = head_scores(query_full, key_cols, bias_terms, head_count)
    row_top = lax.pmax(jnp.max(scores, axis=2), "col")
    weights_exp = jnp.exp(scores - row_top[:, :, None])
    row_sum, summed = lax.psum(
        (jnp.sum(weights_exp, axis=2), weighted_values(weights_exp, value_cols, head_count)), "col"
    )
    attended = divide_heads(summed, row_sum)
    gated = (jax.nn.sigmoid(gate_full.astype(jnp.float32)) * attended).astype(jnp.bfloat16)
    single_out = (single_f + jnp.dot(gated, w_out, preferred_element_type=jnp.float32)).astype(
        jnp.bfloat16
    )
    updated_single = single_out.astype(jnp.float32)
    gained = updated_single * outer_gain
    joint = lax.psum(
        (
            jnp.sum(updated_single, axis=1),
            jnp.sum(updated_single * updated_single, axis=1),
            jnp.dot(gained, w_left, precision=lax.Precision.HIGHEST),
            jnp.dot(gained, w_right, precision=lax.Precision.HIGHEST),
            jnp.dot(outer_gain[None], w_left, precision=lax.Precision.HIGHEST)[0],
            jnp.dot(outer_gain[None], w_right, precision=lax.Precision.HIGHEST)[0],
        ),
        "col",
    )
    out_mean = joint[0] / model_width
    out_inv = lax.rsqrt(joint[1] / model_width - out_mean * out_mean + EPSILON)
    left_full = out_inv[:, None] * (joint[2] - out_mean[:, None] * joint[4][None, :])
    right_full = out_inv[:, None] * (joint[3] - out_mean[:, None] * joint[5][None, :])
    left_rows = left_full.astype(jnp.bfloat16)
    right_rows = right_full.astype(jnp.bfloat16)
    right_cols = broadcast(right_rows, "row", col_place)
    left_mix = jnp.einsum("ip,pqc->iqc", left_rows, w_outer, preferred_element_type=jnp.float32)
    outer = (
        jnp.einsum(
            "iqc,jq->ijc", left_mix, right_cols.astype(jnp.float32), precision=lax.Precision.HIGHEST
        )
        + outer_bias
    )
    outer = outer * (live_query[:, None] * live_keys.astype(jnp.float32)[None, :])[:, :, None]
    updated = pair.astype(jnp.float32) + outer
    flat = updated.reshape(-1, updated.shape[-1])
    total_rows = flat.shape[0]
    piece_rows = math.gcd(total_rows, 1024)
    pieces = flat.reshape(total_rows // piece_rows, piece_rows, flat.shape[1])
    pair_out = lax.map(lambda piece: transition(piece, trans_gain, w_in, w_down), pieces).reshape(
        pair.shape
    )
    return (single_out, pair_out)


def dot_f32(a, b, contract=((1,), (0,))):
    return lax.dot_general(a, b, (contract, ((), ())), preferred_element_type=jnp.float32)


def dot_exact(a, b, contract=((1,), (0,))):
    return lax.dot_general(
        a, b, (contract, ((), ())), precision=lax.Precision.HIGHEST, preferred_element_type=jnp.float32
    )


def split_pair(values):
    high = values.astype(jnp.bfloat16)
    return high, (values - high.astype(jnp.float32)).astype(jnp.bfloat16)


def window(row, start, lanes):
    return pltpu.roll(row, (row.shape[1] - start) % row.shape[1], 1)[:, :lanes]


def as_column(row):
    size = row.shape[1]
    shape = (size, size)
    on_diagonal = lax.broadcasted_iota(jnp.int32, shape, 0) == lax.broadcasted_iota(
        jnp.int32, shape, 1
    )
    spread = jnp.where(on_diagonal, jnp.broadcast_to(row, shape), 0.0)
    return jnp.sum(spread, axis=1, keepdims=True)


def pack_kernel(
    token_ref,
    step_ref,
    scale_ref,
    shift_ref,
    gain_ref,
    left_ref,
    right_ref,
    chain_ref,
    live_ref,
    weight_ref,
    chain_bias_ref,
    outer_bias_ref,
    trans_gain_ref,
    pair_gain_ref,
    single_ref,
    out_ref,
    aux_ref,
):
    del token_ref
    rows, width = single_ref.shape
    keys, channels = rows, aux_ref.shape[1]
    half = rows // 2
    out_ref[:rows, :] = single_ref[...]
    halfway = scale_ref.shape[1] // 2
    ladder = lax.broadcasted_iota(jnp.int32, (16, halfway), 1).astype(jnp.float32)
    freqs = jnp.exp(-math.log(10000.0) * ladder / halfway)
    angles = step_ref[...].astype(jnp.float32) * freqs
    embedded = jnp.concatenate([jnp.sin(angles), jnp.cos(angles)], axis=1).astype(jnp.bfloat16)
    contract = ((1,), (1,))
    mod_scale = dot_f32(embedded, scale_ref[...], contract)[:1]
    mod_shift = dot_f32(embedded, shift_ref[...], contract)[:1]
    gain = jnp.broadcast_to(gain_ref[...], (8, width))
    factors = jnp.concatenate([left_ref[...], right_ref[...]], axis=0)
    factor_sum = dot_exact(gain, factors, contract)[:1]
    filler = jnp.zeros((1, width - factors.shape[0]), jnp.float32)
    sums = jnp.concatenate([factor_sum, filler], axis=1)
    tail = []
    for row in (mod_scale, mod_shift, sums):
        high = row.astype(jnp.bfloat16).astype(jnp.float32)
        tail += [high, row - high]
    tail.append(jnp.zeros((out_ref.shape[0] - rows - len(tail), width), jnp.float32))
    out_ref[rows:, :] = jnp.concatenate(tail, axis=0).astype(jnp.bfloat16)

    chain = chain_ref[...].astype(jnp.float32)
    live = live_ref[...].astype(jnp.float32)
    query_start, key_start = lax.axis_index("row") * rows, lax.axis_index("col") * keys
    chain_column = as_column(window(chain, query_start, rows))
    chain_row = window(chain, key_start, keys)
    distance = jnp.concatenate(
        [chain_column[:half] - chain_row, chain_column[half:] - chain_row], axis=1
    )
    live_keys = window(live, key_start, keys)
    live_terms = jnp.where(live_keys == 1.0, 0.0, MASKED)
    aux_ref[AUX_CHAIN : AUX_CHAIN + half, :] = distance
    aux_ref[AUX_LIVE : AUX_LIVE + 1, :] = jnp.concatenate([live_terms, live_terms], axis=1)
    aux_ref[AUX_VECTORS : AUX_VECTORS + 1, :] = outer_bias_ref[...]
    aux_ref[AUX_VECTORS + 1 : AUX_VECTORS + 2, :] = trans_gain_ref[...]
    aux_ref[AUX_VECTORS + 2 : AUX_VECTORS + 3, :] = pair_gain_ref[...]
    head_count = weight_ref.shape[0]
    aux_ref[AUX_BIAS : AUX_BIAS + 2, :head_count] = chain_bias_ref[...]
    aux_ref[AUX_WEIGHT : AUX_WEIGHT + head_count, :] = weight_ref[...].astype(jnp.float32)
    aux_ref[AUX_KEYS : AUX_KEYS + keys, :] = jnp.broadcast_to(as_column(live_keys), (keys, channels))
    live_queries = as_column(window(live, query_start, rows))
    aux_ref[AUX_QUERIES : AUX_QUERIES + rows, :] = jnp.broadcast_to(live_queries, (rows, channels))


def bias_kernel(aux_ref, pair_ref, out_ref):
    half = out_ref.shape[2]
    keys, channels = pair_ref.shape[1:]
    heads_here = out_ref.shape[1]
    head_count = out_ref.shape[0] * heads_here
    step = 8
    live_terms = aux_ref[AUX_LIVE : AUX_LIVE + 1, :]
    gain = aux_ref[AUX_VECTORS + 2 : AUX_VECTORS + 3, :]
    weight = aux_ref[AUX_WEIGHT : AUX_WEIGHT + 16, :].astype(jnp.bfloat16)
    same_bias = [aux_ref[AUX_BIAS : AUX_BIAS + 1, h : h + 1] for h in range(head_count)]
    other_bias = [aux_ref[AUX_BIAS + 1 : AUX_BIAS + 2, h : h + 1] for h in range(head_count)]
    for start in range(0, half, step):
        parts = []
        for base in (start, half + start):
            block = pair_ref[base : base + step].astype(jnp.float32).reshape(step * keys, channels)
            parts.append(channel_norm(block, gain).astype(jnp.bfloat16))
        normed = []
        for k in range(step):
            normed.append(parts[0][k * keys : (k + 1) * keys])
            normed.append(parts[1][k * keys : (k + 1) * keys])
        terms = dot_f32(weight, jnp.concatenate(normed, axis=0), ((1,), (1,)))
        terms = terms.reshape(terms.shape[0], step, 2 * keys)
        same = aux_ref[AUX_CHAIN + start : AUX_CHAIN + start + step, :] == 0.0
        for head in range(head_count):
            chain_terms = jnp.where(same, same_bias[head], other_bias[head])
            out_ref[head // heads_here, head % heads_here, start : start + step, :] = (
                terms[head] + chain_terms
            ) + live_terms


def project_kernel(*refs):
    count = len(refs) - 8
    blocks = refs[:count]
    query_w, key_w, value_w, gate_w, query_out, kv_out, gate_out, ordered = refs[count:]
    rows, width = query_out.shape
    model_width = query_w.shape[1]
    values = [block[:rows, :].astype(jnp.float32) for block in blocks]
    total = sum(jnp.sum(v, axis=1, keepdims=True) for v in values)
    squares = sum(jnp.sum(v * v, axis=1, keepdims=True) for v in values)
    row_mean = total / model_width
    inv_std = lax.rsqrt(squares / model_width - row_mean * row_mean + EPSILON)
    for k, (block, v) in enumerate(zip(blocks, values)):
        tail = block[rows : rows + 8, :].astype(jnp.float32)
        scale = tail[0:1] + tail[1:2]
        shift = tail[2:3] + tail[3:4]
        normed = (v - row_mean) * inv_std * (1.0 + scale) + shift
        ordered[lax.axis_index("col") ^ k] = normed.astype(jnp.bfloat16)
    normed = jnp.concatenate([ordered[b] for b in range(count)], axis=1)
    contract = ((1,), (1,))
    query_out[...] = dot_f32(normed, query_w[...], contract).astype(jnp.bfloat16)
    kv_out[:, :width] = dot_f32(normed, key_w[...], contract).astype(jnp.bfloat16)
    kv_out[:, width:] = dot_f32(normed, value_w[...], contract).astype(jnp.bfloat16)
    gate_out[...] = dot_f32(normed, gate_w[...], contract).astype(jnp.bfloat16)


def attend_kernel(query_ref, gate_ref, *refs):
    count = (len(refs) - 3) // 2
    kvs = refs[:count]
    biases = refs[count : 2 * count]
    out_ref, kv_all, bias_all = refs[2 * count :]
    rows, width = query_ref.shape
    heads_here = biases[0].shape[0]
    head_size = width // heads_here
    half = rows // 2
    for k in range(count):
        kv_all[pl.ds(pl.multiple_of((lax.axis_index("row") ^ k) * rows, rows), rows), :] = kvs[k][...]
        bias_all[lax.axis_index("col") ^ k] = biases[k][...]
    for head in range(heads_here):
        lanes = slice(head * head_size, (head + 1) * head_size)
        value_lanes = slice(width + head * head_size, width + (head + 1) * head_size)
        raw = dot_f32(query_ref[:, lanes], kv_all[:, lanes], ((1,), (1,)))
        tops = [bias_all[b, head][:, :rows] for b in range(count)]
        lows = [bias_all[b, head][:, rows:] for b in range(count)]
        bias = jnp.concatenate(
            [jnp.concatenate(tops, axis=1), jnp.concatenate(lows, axis=1)], axis=0
        )
        scores = raw * head_size ** (-0.5) + bias
        weights = jnp.exp(scores - jnp.max(scores, axis=1, keepdims=True))
        total = jnp.sum(weights, axis=1, keepdims=True)
        high, low = split_pair(weights)
        values = kv_all[:, value_lanes]
        attended = (dot_f32(high, values) + dot_f32(low, values)) / total
        gate = jax.nn.sigmoid(gate_ref[:, lanes].astype(jnp.float32))
        out_ref[:, lanes] = (gate * attended).astype(jnp.bfloat16)


def output_kernel(single_ref, gain_ref, out_w, left_w, right_w, *refs):
    blocks = refs[:-3]
    single_out, message, ordered = refs[-3:]
    rows, width = single_ref.shape
    half = rows // 2
    for k, block in enumerate(blocks):
        ordered[lax.axis_index("col") ^ k] = block[...]
    gated = jnp.concatenate([ordered[b] for b in range(len(blocks))], axis=1)
    contract = ((1,), (1,))
    total = dot_f32(gated, out_w[...], contract)
    result = (single_ref[...].astype(jnp.float32) + total).astype(jnp.bfloat16)
    single_out[...] = result
    values = result.astype(jnp.float32)
    block_mean = jnp.sum(values, axis=1, keepdims=True) / width
    centered = values - block_mean
    block_var = jnp.sum(centered * centered, axis=1, keepdims=True) / width
    gain_high, gain_low = split_pair(centered * gain_ref[...])
    factor_high, factor_low = split_pair(jnp.concatenate([left_w[...], right_w[...]], axis=0))
    partial = (
        dot_f32(gain_high, factor_high, contract)
        + dot_f32(gain_low, factor_high, contract)
        + dot_f32(gain_high, factor_low, contract)
    )
    lane = lax.broadcasted_iota(jnp.int32, (rows, 128), 1)
    stats = jnp.where(lane == 0, block_mean, jnp.where(lane == 1, block_var, 0.0))
    stats = jnp.transpose(stats)[:8]
    high = stats.astype(jnp.bfloat16).astype(jnp.float32)
    stats = jnp.concatenate([high, stats - high], axis=1).astype(jnp.bfloat16)
    packed = jnp.concatenate([partial[:half], partial[half:]], axis=1).astype(jnp.bfloat16)
    for slot in range(message.shape[0]):
        message[slot, :half, :] = packed
        message[slot, half:, :] = stats


def factor_rows(parts, sums, model_width, factors, which):
    half = parts[0].shape[0] - 8
    lanes = slice(which * factors, (which + 1) * factors)
    far_lanes = slice((which + 2) * factors, (which + 3) * factors)
    means, variances, partials, colsums = [], [], [], []
    for part, tail in zip(parts, sums):
        values = part.astype(jnp.float32)
        stats = values[half:, : 2 * half] + values[half:, 2 * half :]
        means.append(stats[0:1])
        variances.append(stats[1:2])
        partials.append(
            jnp.concatenate([values[:half, lanes], values[:half, far_lanes]], axis=0)
        )
        colsums.append(tail[:, lanes])
    count = len(parts)
    mean = sum(means) / count
    spread = sum(v + (m - mean) * (m - mean) for v, m in zip(variances, means)) / count
    inv_std = as_column(lax.rsqrt(spread + EPSILON))
    shifts = [as_column(m - mean) for m in means]
    total = sum(p + m * s for p, m, s in zip(partials, shifts, colsums))
    return (inv_std * total).astype(jnp.bfloat16)


def update_kernel(
    single_ref,
    message_ref,
    pair_ref,
    aux_ref,
    outer_w_ref,
    w_in_ref,
    w_down_ref,
    *refs,
):
    blocks = refs[:-8]
    single_hbm, out_hbm, out_ref, mix_ref, right_ref, gate_w_ref, semaphore, semaphores = refs[-8:]
    rows, keys, channels = pair_ref.shape
    count = len(blocks)
    factors = outer_w_ref.shape[0]
    halfway = w_down_ref.shape[0]
    steps = semaphores.shape[0]
    step_rows = rows // steps
    single_copy = pltpu.make_async_copy(single_ref, single_hbm, semaphore)
    single_copy.start()

    sums = []
    for block in blocks:
        tail = block[rows : rows + 8, :].astype(jnp.float32)
        sums.append(tail[4:5] + tail[5:6])
    model_width = blocks[0].shape[1] * count
    lefts = [message_ref[lax.axis_index("row") * count + (lax.axis_index("col") ^ k)] for k in range(count)]
    rights = [message_ref[lax.axis_index("col") * count + (lax.axis_index("col") ^ k)] for k in range(count)]
    left = factor_rows(lefts, sums, model_width, factors, 0)
    right = factor_rows(rights, sums, model_width, factors, 1)
    live_keys = aux_ref[AUX_KEYS : AUX_KEYS + keys, :]
    live_queries = aux_ref[AUX_QUERIES : AUX_QUERIES + rows, :]
    spare = right_ref.shape[1] - 2 * factors
    live_right = live_keys[:, :factors].astype(jnp.bfloat16)
    right = right * live_right
    right_ref[...] = jnp.concatenate([right, right, live_right[:, :spare]], axis=1)
    left = left * live_queries[:, :factors].astype(jnp.bfloat16)
    mix = dot_f32(left, outer_w_ref[...]).reshape(rows, factors, channels)
    high, low = split_pair(mix)
    mix_ref[:, :factors, :] = high
    mix_ref[:, factors : 2 * factors, :] = low
    bias = aux_ref[AUX_VECTORS : AUX_VECTORS + 1, :]
    bias_high = bias.astype(jnp.bfloat16).astype(jnp.float32)
    pick = lax.broadcasted_iota(jnp.int32, (spare, channels), 0)
    bias_rows = jnp.where(pick == 0, bias_high, jnp.where(pick == 1, bias - bias_high, 0.0))
    mix_ref[:, 2 * factors :, :] = (live_queries[:, None, :] * bias_rows[None]).astype(jnp.bfloat16)
    gate_w_ref[...] = w_in_ref[:, :halfway] * jnp.asarray(0.5, w_in_ref.dtype)

    def copy_out(step):
        block = pl.ds(step * step_rows, step_rows)
        return pltpu.make_async_copy(out_ref.at[block], out_hbm.at[block], semaphores.at[step])

    def front(start, step_rows):
        mixes = [mix_ref[start + i] for i in range(step_rows)]
        outers = dot_f32(right_ref[...], jnp.concatenate(mixes, axis=1))
        pieces = []
        for i in range(step_rows):
            outer = outers[:, i * channels : (i + 1) * channels]
            pieces.append(pair_ref[start + i].astype(jnp.float32) + outer)
        flat = jnp.concatenate(pieces, axis=0)
        normed = channel_norm(flat, aux_ref[AUX_VECTORS + 1 : AUX_VECTORS + 2, :]).astype(jnp.bfloat16)
        gate = dot_f32(normed, gate_w_ref[...])
        up = dot_f32(normed, w_in_ref[:, halfway:])
        return flat, ((gate + gate * jnp.tanh(gate)) * up).astype(jnp.bfloat16)

    def back(step, flat, hidden):
        result = flat + dot_f32(hidden, w_down_ref[...])
        block = slice(step * step_rows, (step + 1) * step_rows)
        out_ref[block] = result.astype(jnp.bfloat16).reshape(step_rows, keys, channels)
        copy_out(step).start()

    flat, hidden = front(0, rows)
    for step in range(steps):
        part = slice(step * step_rows * keys, (step + 1) * step_rows * keys)
        back(step, flat[part], hidden[part])
    for step in range(steps):
        copy_out(step).wait()
    single_copy.wait()


def token_kernel(token_ref):
    token_ref[...] = jnp.zeros(token_ref.shape, token_ref.dtype)


def local_call(
    kernel, operands, outs, name, scratch=(), hbm_out=False, grant=24 * 2**20, flops=0
):
    out_space = pltpu.HBM if hbm_out else pltpu.VMEM
    out_specs = [pl.BlockSpec(memory_space=out_space) for _ in outs]
    if len(outs) == 1:
        outs, out_specs = outs[0], out_specs[0]
    return pl.pallas_call(
        kernel,
        out_shape=outs,
        in_specs=[pl.BlockSpec(memory_space=pltpu.VMEM) for _ in operands],
        out_specs=out_specs,
        scratch_shapes=list(scratch),
        compiler_params=pltpu.CompilerParams(vmem_limit_bytes=grant),
        cost_estimate=pl.CostEstimate(flops=flops, bytes_accessed=2**18, transcendentals=0),
        name=name,
    )(*operands)


def exchange(array, axis, count):
    return [
        lax.ppermute(array, axis, [(i, i ^ k) for i in range(count)]) for k in range(1, count)
    ]


def headwise_body(
    single,
    pair,
    chain,
    live,
    step_index,
    time_scale,
    time_shift,
    w_query,
    w_key,
    w_value,
    w_gate,
    w_out,
    pair_gain,
    bias_weight,
    chain_bias,
    outer_gain,
    w_left,
    w_right,
    w_outer,
    outer_bias,
    trans_gain,
    w_in,
    w_down,
):
    bf16, f32 = jnp.bfloat16, jnp.float32
    rows, width = single.shape
    keys, channels = pair.shape[1:]
    half = rows // 2
    head_count = chain_bias.shape[1]
    count = lax.axis_size("col")
    heads_here = head_count // count
    factors = w_left.shape[1]
    col_place = lax.axis_index("col")
    shape = jax.ShapeDtypeStruct
    token = local_call(token_kernel, (), [shape((8, 128), f32)], "token", flops=10**10)
    packed, aux = local_call(
        pack_kernel,
        (
            token,
            step_index[None],
            time_scale.T,
            time_shift.T,
            outer_gain[None],
            w_left.T,
            w_right.T,
            chain[None],
            live[None],
            bias_weight.T,
            chain_bias,
            outer_bias[None],
            trans_gain[None],
            pair_gain[None],
            single,
        ),
        [shape((rows + 16, width), bf16), shape((AUX_ROWS, channels), f32)],
        "pack",
        flops=10**10,
    )
    blocks = [packed] + exchange(packed, "col", count)

    bias = local_call(
        bias_kernel,
        (aux, pair),
        [shape((count, heads_here, half, 2 * keys), f32)],
        "pair_bias",
        flops=10**10,
    )
    pieces = [lax.dynamic_index_in_dim(bias, col_place ^ k, 0, keepdims=False) for k in range(count)]
    biases = pieces[:1] + [
        lax.ppermute(pieces[k], "col", [(i, i ^ k) for i in range(count)]) for k in range(1, count)
    ]

    query, kv, gate = local_call(
        project_kernel,
        (*blocks, w_query.T, w_key.T, w_value.T, w_gate.T),
        [shape((rows, width), bf16), shape((rows, 2 * width), bf16), shape((rows, width), bf16)],
        "project",
        scratch=(pltpu.VMEM((count, rows, width), bf16),),
        flops=10**8,
    )
    kvs = [kv] + exchange(kv, "row", count)
    gated = local_call(
        attend_kernel,
        (query, gate, *kvs, *biases),
        [shape((rows, width), bf16)],
        "attend",
        scratch=(
            pltpu.VMEM((count * rows, 2 * width), bf16),
            pltpu.VMEM((count, heads_here, half, 2 * keys), f32),
        ),
        flops=10**8,
    )
    gateds = [gated] + exchange(gated, "col", count)
    result, message = local_call(
        output_kernel,
        (single, outer_gain[None], w_out.T, w_left.T, w_right.T, *gateds),
        [shape((rows, width), bf16), shape((count * count, half + 8, 2 * keys), bf16)],
        "project_out",
        scratch=(pltpu.VMEM((count, rows, width), bf16),),
        flops=10**7,
    )
    outer_flat = w_outer.reshape(factors, factors * channels)
    message, outer_flat = lax.optimization_barrier((message, outer_flat))
    message = lax.all_to_all(message, ("row", "col"), 0, 0)

    steps = 4
    single_out, pair_out = local_call(
        update_kernel,
        (
            result,
            message,
            pair,
            aux,
            outer_flat,
            w_in,
            w_down,
            *blocks,
        ),
        [shape((rows, width), bf16), shape(pair.shape, bf16)],
        "pair_update",
        scratch=(
            pltpu.VMEM(pair.shape, bf16),
            pltpu.VMEM((rows, 2 * factors + 16, channels), bf16),
            pltpu.VMEM((keys, 2 * factors + 16), bf16),
            pltpu.VMEM((w_in.shape[0], w_down.shape[0]), bf16),
            pltpu.SemaphoreType.DMA,
            pltpu.SemaphoreType.DMA((steps,)),
        ),
        hbm_out=True,
        flops=2 * 10**9,
    )
    return (single_out, pair_out)


def pick_body(mesh):
    rows, cols = mesh.shape["row"], mesh.shape["col"]

    def chosen(*arrays):
        single, pair, chain_bias = arrays[0], arrays[1], arrays[14]
        fits = (
            rows == cols
            and cols & (cols - 1) == 0
            and chain_bias.shape[1] % cols == 0
            and single.shape[0] == pair.shape[1] == 64
            and 4 * arrays[16].shape[1] == pair.shape[2]
            and chain_bias.shape[1] <= AUX_ROWS - AUX_WEIGHT
            and pair.shape[2] == 128
        )
        return headwise_body(*arrays) if fits else body(*arrays)

    return chosen


def solution(mesh):
    in_specs = (
        P(("groups", "row"), "col"),
        P(("groups", "row"), "col", None),
        P("groups"),
        P("groups"),
        P("groups"),
        P(None, "col"),
        P(None, "col"),
        P(None, "col"),
        P(None, "col"),
        P(None, "col"),
        P(None, "col"),
        P(None, "col"),
        P(),
        P(),
        P(),
        P("col"),
        P("col", None),
        P("col", None),
        P(),
        P(),
        P(),
        P(),
        P(),
    )
    out_specs = (P(("groups", "row"), "col"), P(("groups", "row"), "col", None))
    return jax.shard_map(
        pick_body(mesh), mesh=mesh, in_specs=in_specs, out_specs=out_specs, check_vma=False)
```

```python
import math

import jax
import jax.numpy as jnp
from jax import lax
from jax.experimental import pallas as pl
from jax.experimental.pallas import tpu as pltpu
from jax.sharding import PartitionSpec as P

EPSILON = 1e-05
MASKED = -1000000000.0
AUX_CHAIN = 0
AUX_LIVE = 32
AUX_VECTORS = 40
AUX_BIAS = 48
AUX_KEYS = 56
AUX_QUERIES = 120
AUX_WEIGHT = 184
AUX_ROWS = 200


def broadcast(array, axis, root):
    mine = lax.axis_index(axis) == root
    return lax.psum(jnp.where(mine, array, jnp.zeros_like(array)), axis)


def channel_norm(values, gain):
    row_mean = jnp.mean(values, axis=-1, keepdims=True)
    spread = jnp.mean(values * values, axis=-1, keepdims=True) - row_mean * row_mean
    return (values - row_mean) * lax.rsqrt(spread + EPSILON) * gain


def time_embed(step_index, count):
    halfway = count // 2
    ladder = jnp.arange(halfway).astype(jnp.float32)
    freqs = jnp.exp(-math.log(10000.0) * ladder / halfway)
    angles = step_index[0].astype(jnp.float32) * freqs
    return jnp.concatenate([jnp.sin(angles), jnp.cos(angles)])


def head_scores(query_rows, key_rows, bias_terms, head_count):
    query_heads = query_rows.reshape(query_rows.shape[0], head_count, -1)
    key_heads = key_rows.reshape(key_rows.shape[0], head_count, -1)
    raw = jnp.einsum("qhd,khd->hqk", query_heads, key_heads, preferred_element_type=jnp.float32)
    return raw * query_heads.shape[2] ** (-0.5) + bias_terms


def weighted_values(weights_exp, value_rows, head_count):
    value_heads = value_rows.reshape(value_rows.shape[0], head_count, -1).astype(jnp.float32)
    summed = jnp.einsum("hqk,khd->qhd", weights_exp, value_heads, precision=lax.Precision.HIGHEST)
    return summed.reshape(summed.shape[0], -1)


def divide_heads(summed, totals):
    row_count = summed.shape[0]
    head_count = totals.shape[0]
    return (summed.reshape(row_count, head_count, -1) / totals.T[:, :, None]).reshape(row_count, -1)


def transition(flat, gain, w_in, w_down):
    normed = channel_norm(flat, gain).astype(jnp.bfloat16)
    mixed = jnp.dot(normed, w_in, preferred_element_type=jnp.float32)
    halfway = w_down.shape[0]
    hidden = (jax.nn.silu(mixed[:, :halfway]) * mixed[:, halfway:]).astype(jnp.bfloat16)
    return (flat + jnp.dot(hidden, w_down, preferred_element_type=jnp.float32)).astype(jnp.bfloat16)


def body(
    single,
    pair,
    chain,
    live,
    step_index,
    time_scale,
    time_shift,
    w_query,
    w_key,
    w_value,
    w_gate,
    w_out,
    pair_gain,
    bias_weight,
    chain_bias,
    outer_gain,
    w_left,
    w_right,
    w_outer,
    outer_bias,
    trans_gain,
    w_in,
    w_down,
):
    block_rows = single.shape[0]
    model_width = w_query.shape[0]
    head_count = chain_bias.shape[1]
    row_place = lax.axis_index("row")
    col_place = lax.axis_index("col")
    query_start = row_place * block_rows
    key_start = col_place * block_rows
    chain_query = lax.dynamic_slice_in_dim(chain, query_start, block_rows, 0)
    chain_key = lax.dynamic_slice_in_dim(chain, key_start, block_rows, 0)
    live_query = lax.dynamic_slice_in_dim(live, query_start, block_rows, 0).astype(jnp.float32)
    live_keys = lax.dynamic_slice_in_dim(live, key_start, block_rows, 0)
    single_f = single.astype(jnp.float32)
    totals = lax.psum((jnp.sum(single_f, axis=1), jnp.sum(single_f * single_f, axis=1)), "col")
    row_mean = totals[0] / model_width
    inv_std = lax.rsqrt(totals[1] / model_width - row_mean * row_mean + EPSILON)
    embedded = time_embed(step_index, time_scale.shape[0]).astype(jnp.bfloat16)
    mod_scale = jnp.dot(embedded[None], time_scale, preferred_element_type=jnp.float32)[0]
    mod_shift = jnp.dot(embedded[None], time_shift, preferred_element_type=jnp.float32)[0]
    normed = (
        (single_f - row_mean[:, None]) * inv_std[:, None] * (1.0 + mod_scale) + mod_shift
    ).astype(jnp.bfloat16)
    normed_full = lax.all_gather(normed, "col", axis=1, tiled=True)
    query_part = jnp.dot(normed_full, w_query, preferred_element_type=jnp.float32).astype(
        jnp.bfloat16
    )
    key_part = jnp.dot(normed_full, w_key, preferred_element_type=jnp.float32).astype(jnp.bfloat16)
    value_part = jnp.dot(normed_full, w_value, preferred_element_type=jnp.float32).astype(
        jnp.bfloat16
    )
    gate_part = jnp.dot(normed_full, w_gate, preferred_element_type=jnp.float32).astype(
        jnp.bfloat16
    )
    query_full, key_full, value_full, gate_full = (
        lax.all_gather(query_part, "col", axis=1, tiled=True),
        lax.all_gather(key_part, "col", axis=1, tiled=True),
        lax.all_gather(value_part, "col", axis=1, tiled=True),
        lax.all_gather(gate_part, "col", axis=1, tiled=True),
    )
    key_cols, value_cols = (
        broadcast(key_full, "row", col_place),
        broadcast(value_full, "row", col_place),
    )
    pair_normed = channel_norm(pair.astype(jnp.float32), pair_gain).astype(jnp.bfloat16)
    bias_terms = jnp.einsum(
        "qkc,ch->hqk", pair_normed, bias_weight, preferred_element_type=jnp.float32
    )
    same_chain = chain_query[:, None] == chain_key[None, :]
    chain_terms = jnp.where(
        same_chain[None], chain_bias[0][:, None, None], chain_bias[1][:, None, None]
    )
    live_terms = jnp.where(live_keys == 1, 0.0, MASKED).astype(jnp.float32)
    bias_terms = bias_terms + chain_terms + live_terms[None, None, :]
    scores = head_scores(query_full, key_cols, bias_terms, head_count)
    row_top = lax.pmax(jnp.max(scores, axis=2), "col")
    weights_exp = jnp.exp(scores - row_top[:, :, None])
    row_sum, summed = lax.psum(
        (jnp.sum(weights_exp, axis=2), weighted_values(weights_exp, value_cols, head_count)), "col"
    )
    attended = divide_heads(summed, row_sum)
    gated = (jax.nn.sigmoid(gate_full.astype(jnp.float32)) * attended).astype(jnp.bfloat16)
    single_out = (single_f + jnp.dot(gated, w_out, preferred_element_type=jnp.float32)).astype(
        jnp.bfloat16
    )
    updated_single = single_out.astype(jnp.float32)
    gained = updated_single * outer_gain
    joint = lax.psum(
        (
            jnp.sum(updated_single, axis=1),
            jnp.sum(updated_single * updated_single, axis=1),
            jnp.dot(gained, w_left, precision=lax.Precision.HIGHEST),
            jnp.dot(gained, w_right, precision=lax.Precision.HIGHEST),
            jnp.dot(outer_gain[None], w_left, precision=lax.Precision.HIGHEST)[0],
            jnp.dot(outer_gain[None], w_right, precision=lax.Precision.HIGHEST)[0],
        ),
        "col",
    )
    out_mean = joint[0] / model_width
    out_inv = lax.rsqrt(joint[1] / model_width - out_mean * out_mean + EPSILON)
    left_full = out_inv[:, None] * (joint[2] - out_mean[:, None] * joint[4][None, :])
    right_full = out_inv[:, None] * (joint[3] - out_mean[:, None] * joint[5][None, :])
    left_rows = left_full.astype(jnp.bfloat16)
    right_rows = right_full.astype(jnp.bfloat16)
    right_cols = broadcast(right_rows, "row", col_place)
    left_mix = jnp.einsum("ip,pqc->iqc", left_rows, w_outer, preferred_element_type=jnp.float32)
    outer = (
        jnp.einsum(
            "iqc,jq->ijc", left_mix, right_cols.astype(jnp.float32), precision=lax.Precision.HIGHEST
        )
        + outer_bias
    )
    outer = outer * (live_query[:, None] * live_keys.astype(jnp.float32)[None, :])[:, :, None]
    updated = pair.astype(jnp.float32) + outer
    flat = updated.reshape(-1, updated.shape[-1])
    total_rows = flat.shape[0]
    piece_rows = math.gcd(total_rows, 1024)
    pieces = flat.reshape(total_rows // piece_rows, piece_rows, flat.shape[1])
    pair_out = lax.map(lambda piece: transition(piece, trans_gain, w_in, w_down), pieces).reshape(
        pair.shape
    )
    return (single_out, pair_out)


def dot_f32(a, b, contract=((1,), (0,))):
    return lax.dot_general(a, b, (contract, ((), ())), preferred_element_type=jnp.float32)


def dot_exact(a, b, contract=((1,), (0,))):
    return lax.dot_general(
        a, b, (contract, ((), ())), precision=lax.Precision.HIGHEST, preferred_element_type=jnp.float32
    )


def split_pair(values):
    high = values.astype(jnp.bfloat16)
    return high, (values - high.astype(jnp.float32)).astype(jnp.bfloat16)


def window(row, start, lanes):
    return pltpu.roll(row, (row.shape[1] - start) % row.shape[1], 1)[:, :lanes]


def as_column(row):
    size = row.shape[1]
    shape = (size, size)
    on_diagonal = lax.broadcasted_iota(jnp.int32, shape, 0) == lax.broadcasted_iota(
        jnp.int32, shape, 1
    )
    spread = jnp.where(on_diagonal, jnp.broadcast_to(row, shape), 0.0)
    return jnp.sum(spread, axis=1, keepdims=True)


def pack_kernel(
    token_ref,
    step_ref,
    scale_ref,
    shift_ref,
    gain_ref,
    left_ref,
    right_ref,
    chain_ref,
    live_ref,
    weight_ref,
    chain_bias_ref,
    outer_bias_ref,
    trans_gain_ref,
    pair_gain_ref,
    single_ref,
    out_ref,
    aux_ref,
):
    del token_ref
    rows, width = single_ref.shape
    keys, channels = rows, aux_ref.shape[1]
    half = rows // 2
    out_ref[:rows, :] = single_ref[...]
    halfway = scale_ref.shape[1] // 2
    ladder = lax.broadcasted_iota(jnp.int32, (16, halfway), 1).astype(jnp.float32)
    freqs = jnp.exp(-math.log(10000.0) * ladder / halfway)
    angles = step_ref[...].astype(jnp.float32) * freqs
    embedded = jnp.concatenate([jnp.sin(angles), jnp.cos(angles)], axis=1).astype(jnp.bfloat16)
    contract = ((1,), (1,))
    mod_scale = dot_f32(embedded, scale_ref[...], contract)[:1]
    mod_shift = dot_f32(embedded, shift_ref[...], contract)[:1]
    gain = jnp.broadcast_to(gain_ref[...], (8, width))
    factors = jnp.concatenate([left_ref[...], right_ref[...]], axis=0)
    factor_sum = dot_exact(gain, factors, contract)[:1]
    filler = jnp.zeros((1, width - factors.shape[0]), jnp.float32)
    sums = jnp.concatenate([factor_sum, filler], axis=1)
    tail = []
    for row in (mod_scale, mod_shift, sums):
        high = row.astype(jnp.bfloat16).astype(jnp.float32)
        tail += [high, row - high]
    tail.append(jnp.zeros((out_ref.shape[0] - rows - len(tail), width), jnp.float32))
    out_ref[rows:, :] = jnp.concatenate(tail, axis=0).astype(jnp.bfloat16)

    chain = chain_ref[...].astype(jnp.float32)
    live = live_ref[...].astype(jnp.float32)
    query_start, key_start = lax.axis_index("row") * rows, lax.axis_index("col") * keys
    chain_column = as_column(window(chain, query_start, rows))
    chain_row = window(chain, key_start, keys)
    distance = jnp.concatenate(
        [chain_column[:half] - chain_row, chain_column[half:] - chain_row], axis=1
    )
    live_keys = window(live, key_start, keys)
    live_terms = jnp.where(live_keys == 1.0, 0.0, MASKED)
    aux_ref[AUX_CHAIN : AUX_CHAIN + half, :] = distance
    aux_ref[AUX_LIVE : AUX_LIVE + 1, :] = jnp.concatenate([live_terms, live_terms], axis=1)
    aux_ref[AUX_VECTORS : AUX_VECTORS + 1, :] = outer_bias_ref[...]
    aux_ref[AUX_VECTORS + 1 : AUX_VECTORS + 2, :] = trans_gain_ref[...]
    aux_ref[AUX_VECTORS + 2 : AUX_VECTORS + 3, :] = pair_gain_ref[...]
    head_count = weight_ref.shape[0]
    aux_ref[AUX_BIAS : AUX_BIAS + 2, :head_count] = chain_bias_ref[...]
    aux_ref[AUX_WEIGHT : AUX_WEIGHT + head_count, :] = weight_ref[...].astype(jnp.float32)
    aux_ref[AUX_KEYS : AUX_KEYS + keys, :] = jnp.broadcast_to(as_column(live_keys), (keys, channels))
    live_queries = as_column(window(live, query_start, rows))
    aux_ref[AUX_QUERIES : AUX_QUERIES + rows, :] = jnp.broadcast_to(live_queries, (rows, channels))


def bias_kernel(aux_ref, pair_ref, out_ref):
    half = out_ref.shape[2]
    keys, channels = pair_ref.shape[1:]
    heads_here = out_ref.shape[1]
    head_count = out_ref.shape[0] * heads_here
    step = 8
    live_terms = aux_ref[AUX_LIVE : AUX_LIVE + 1, :]
    gain = aux_ref[AUX_VECTORS + 2 : AUX_VECTORS + 3, :]
    weight = aux_ref[AUX_WEIGHT : AUX_WEIGHT + 16, :].astype(jnp.bfloat16)
    same_bias = [aux_ref[AUX_BIAS : AUX_BIAS + 1, h : h + 1] for h in range(head_count)]
    other_bias = [aux_ref[AUX_BIAS + 1 : AUX_BIAS + 2, h : h + 1] for h in range(head_count)]
    for start in range(0, half, step):
        parts = []
        for base in (start, half + start):
            block = pair_ref[base : base + step].astype(jnp.float32).reshape(step * keys, channels)
            parts.append(channel_norm(block, gain).astype(jnp.bfloat16))
        normed = []
        for k in range(step):
            normed.append(parts[0][k * keys : (k + 1) * keys])
            normed.append(parts[1][k * keys : (k + 1) * keys])
        terms = dot_f32(weight, jnp.concatenate(normed, axis=0), ((1,), (1,)))
        terms = terms.reshape(terms.shape[0], step, 2 * keys)
        same = aux_ref[AUX_CHAIN + start : AUX_CHAIN + start + step, :] == 0.0
        for head in range(head_count):
            chain_terms = jnp.where(same, same_bias[head], other_bias[head])
            out_ref[head // heads_here, head % heads_here, start : start + step, :] = (
                terms[head] + chain_terms
            ) + live_terms


def project_kernel(*refs):
    count = len(refs) - 8
    blocks = refs[:count]
    query_w, key_w, value_w, gate_w, query_out, kv_out, gate_out, ordered = refs[count:]
    rows, width = query_out.shape
    model_width = query_w.shape[1]
    values = [block[:rows, :].astype(jnp.float32) for block in blocks]
    total = sum(jnp.sum(v, axis=1, keepdims=True) for v in values)
    squares = sum(jnp.sum(v * v, axis=1, keepdims=True) for v in values)
    row_mean = total / model_width
    inv_std = lax.rsqrt(squares / model_width - row_mean * row_mean + EPSILON)
    for k, (block, v) in enumerate(zip(blocks, values)):
        tail = block[rows : rows + 8, :].astype(jnp.float32)
        scale = tail[0:1] + tail[1:2]
        shift = tail[2:3] + tail[3:4]
        normed = (v - row_mean) * inv_std * (1.0 + scale) + shift
        ordered[lax.axis_index("col") ^ k] = normed.astype(jnp.bfloat16)
    normed = jnp.concatenate([ordered[b] for b in range(count)], axis=1)
    contract = ((1,), (1,))
    query_out[...] = dot_f32(normed, query_w[...], contract).astype(jnp.bfloat16)
    kv_out[:, :width] = dot_f32(normed, key_w[...], contract).astype(jnp.bfloat16)
    kv_out[:, width:] = dot_f32(normed, value_w[...], contract).astype(jnp.bfloat16)
    gate_out[...] = dot_f32(normed, gate_w[...], contract).astype(jnp.bfloat16)


def attend_kernel(query_ref, gate_ref, *refs):
    count = (len(refs) - 3) // 2
    kvs = refs[:count]
    biases = refs[count : 2 * count]
    out_ref, kv_all, bias_all = refs[2 * count :]
    rows, width = query_ref.shape
    heads_here = biases[0].shape[0]
    head_size = width // heads_here
    half = rows // 2
    for k in range(count):
        kv_all[pl.ds(pl.multiple_of((lax.axis_index("row") ^ k) * rows, rows), rows), :] = kvs[k][...]
        bias_all[lax.axis_index("col") ^ k] = biases[k][...]
    for head in range(heads_here):
        lanes = slice(head * head_size, (head + 1) * head_size)
        value_lanes = slice(width + head * head_size, width + (head + 1) * head_size)
        raw = dot_f32(query_ref[:, lanes], kv_all[:, lanes], ((1,), (1,)))
        tops = [bias_all[b, head][:, :rows] for b in range(count)]
        lows = [bias_all[b, head][:, rows:] for b in range(count)]
        bias = jnp.concatenate(
            [jnp.concatenate(tops, axis=1), jnp.concatenate(lows, axis=1)], axis=0
        )
        scores = raw * head_size ** (-0.5) + bias
        weights = jnp.exp(scores - jnp.max(scores, axis=1, keepdims=True))
        total = jnp.sum(weights, axis=1, keepdims=True)
        high, low = split_pair(weights)
        values = kv_all[:, value_lanes]
        attended = (dot_f32(high, values) + dot_f32(low, values)) / total
        gate = jax.nn.sigmoid(gate_ref[:, lanes].astype(jnp.float32))
        gated = (gate * attended).astype(jnp.bfloat16)
        top = (head // 2) * rows
        if head == heads_here - 1 and heads_here % 2 == 1:
            out_ref[top : top + half, :] = jnp.concatenate([gated[:half], gated[half:]], axis=1)
        else:
            side = (head % 2) * head_size
            out_ref[top : top + rows, side : side + head_size] = gated


def unfold(block, rows, width):
    half = rows // 2
    lanes = block.shape[1]
    pieces = [block[k * rows : (k + 1) * rows] for k in range(width // lanes)]
    if width % lanes:
        last = block[width // lanes * rows :]
        pieces.append(jnp.concatenate([last[:, : lanes // 2], last[:, lanes // 2 :]], axis=0))
    return jnp.concatenate(pieces, axis=1)


def output_kernel(single_ref, gain_ref, out_w, left_w, right_w, *refs):
    blocks = refs[:-3]
    single_out, message, ordered = refs[-3:]
    rows, width = single_ref.shape
    half = rows // 2
    for k, block in enumerate(blocks):
        ordered[lax.axis_index("col") ^ k] = block[...]
    gated = jnp.concatenate(
        [unfold(ordered[b], rows, width) for b in range(len(blocks))], axis=1
    )
    contract = ((1,), (1,))
    total = dot_f32(gated, out_w[...], contract)
    result = (single_ref[...].astype(jnp.float32) + total).astype(jnp.bfloat16)
    single_out[...] = result
    values = result.astype(jnp.float32)
    block_mean = jnp.sum(values, axis=1, keepdims=True) / width
    centered = values - block_mean
    block_var = jnp.sum(centered * centered, axis=1, keepdims=True) / width
    gain_high, gain_low = split_pair(centered * gain_ref[...])
    factor_high, factor_low = split_pair(jnp.concatenate([left_w[...], right_w[...]], axis=0))
    partial = (
        dot_f32(gain_high, factor_high, contract)
        + dot_f32(gain_low, factor_high, contract)
        + dot_f32(gain_high, factor_low, contract)
    )
    lane = lax.broadcasted_iota(jnp.int32, (rows, 128), 1)
    stats = jnp.where(lane == 0, block_mean, jnp.where(lane == 1, block_var, 0.0))
    stats = jnp.transpose(stats)[:8]
    high = stats.astype(jnp.bfloat16).astype(jnp.float32)
    stats = jnp.concatenate([high, stats - high], axis=1).astype(jnp.bfloat16)
    packed = jnp.concatenate([partial[:half], partial[half:]], axis=1).astype(jnp.bfloat16)
    for slot in range(message.shape[0]):
        message[slot, :half, :] = packed
        message[slot, half:, :] = stats


def factor_rows(parts, sums, model_width, factors, which):
    half = parts[0].shape[0] - 8
    lanes = slice(which * factors, (which + 1) * factors)
    far_lanes = slice((which + 2) * factors, (which + 3) * factors)
    means, variances, partials, colsums = [], [], [], []
    for part, tail in zip(parts, sums):
        values = part.astype(jnp.float32)
        stats = values[half:, : 2 * half] + values[half:, 2 * half :]
        means.append(stats[0:1])
        variances.append(stats[1:2])
        partials.append(
            jnp.concatenate([values[:half, lanes], values[:half, far_lanes]], axis=0)
        )
        colsums.append(tail[:, lanes])
    count = len(parts)
    mean = sum(means) / count
    spread = sum(v + (m - mean) * (m - mean) for v, m in zip(variances, means)) / count
    inv_std = as_column(lax.rsqrt(spread + EPSILON))
    shifts = [as_column(m - mean) for m in means]
    total = sum(p + m * s for p, m, s in zip(partials, shifts, colsums))
    return (inv_std * total).astype(jnp.bfloat16)


def update_kernel(
    single_ref,
    message_ref,
    pair_ref,
    aux_ref,
    outer_w_ref,
    w_in_ref,
    w_down_ref,
    *refs,
):
    blocks = refs[:-8]
    single_hbm, out_hbm, out_ref, mix_ref, right_ref, gate_w_ref, semaphore, semaphores = refs[-8:]
    rows, keys, channels = pair_ref.shape
    count = len(blocks)
    factors = outer_w_ref.shape[0]
    halfway = w_down_ref.shape[0]
    steps = semaphores.shape[0]
    step_rows = rows // steps
    single_copy = pltpu.make_async_copy(single_ref, single_hbm, semaphore)
    single_copy.start()

    sums = []
    for block in blocks:
        tail = block[rows : rows + 8, :].astype(jnp.float32)
        sums.append(tail[4:5] + tail[5:6])
    model_width = blocks[0].shape[1] * count
    lefts = [message_ref[lax.axis_index("row") * count + (lax.axis_index("col") ^ k)] for k in range(count)]
    rights = [message_ref[lax.axis_index("col") * count + (lax.axis_index("col") ^ k)] for k in range(count)]
    left = factor_rows(lefts, sums, model_width, factors, 0)
    right = factor_rows(rights, sums, model_width, factors, 1)
    live_keys = aux_ref[AUX_KEYS : AUX_KEYS + keys, :]
    live_queries = aux_ref[AUX_QUERIES : AUX_QUERIES + rows, :]
    spare = right_ref.shape[1] - 2 * factors
    live_right = live_keys[:, :factors].astype(jnp.bfloat16)
    right = right * live_right
    right_ref[...] = jnp.concatenate([right, right, live_right[:, :spare]], axis=1)
    left = left * live_queries[:, :factors].astype(jnp.bfloat16)
    mix = dot_f32(left, outer_w_ref[...]).reshape(rows, factors, channels)
    high, low = split_pair(mix)
    mix_ref[:, :factors, :] = high
    mix_ref[:, factors : 2 * factors, :] = low
    bias = aux_ref[AUX_VECTORS : AUX_VECTORS + 1, :]
    bias_high = bias.astype(jnp.bfloat16).astype(jnp.float32)
    pick = lax.broadcasted_iota(jnp.int32, (spare, channels), 0)
    bias_rows = jnp.where(pick == 0, bias_high, jnp.where(pick == 1, bias - bias_high, 0.0))
    mix_ref[:, 2 * factors :, :] = (live_queries[:, None, :] * bias_rows[None]).astype(jnp.bfloat16)
    gate_w_ref[...] = w_in_ref[:, :halfway] * jnp.asarray(0.5, w_in_ref.dtype)

    def copy_out(step):
        block = pl.ds(step * step_rows, step_rows)
        return pltpu.make_async_copy(out_ref.at[block], out_hbm.at[block], semaphores.at[step])

    def front(start, step_rows):
        mixes = [mix_ref[start + i] for i in range(step_rows)]
        outers = dot_f32(right_ref[...], jnp.concatenate(mixes, axis=1))
        pieces = []
        for i in range(step_rows):
            outer = outers[:, i * channels : (i + 1) * channels]
            pieces.append(pair_ref[start + i].astype(jnp.float32) + outer)
        flat = jnp.concatenate(pieces, axis=0)
        normed = channel_norm(flat, aux_ref[AUX_VECTORS + 1 : AUX_VECTORS + 2, :]).astype(jnp.bfloat16)
        gate = dot_f32(normed, gate_w_ref[...])
        up = dot_f32(normed, w_in_ref[:, halfway:])
        return flat, ((gate + gate * jnp.tanh(gate)) * up).astype(jnp.bfloat16)

    def back(step, flat, hidden):
        result = flat + dot_f32(hidden, w_down_ref[...])
        block = slice(step * step_rows, (step + 1) * step_rows)
        out_ref[block] = result.astype(jnp.bfloat16).reshape(step_rows, keys, channels)
        copy_out(step).start()

    flat, hidden = front(0, rows)
    for step in range(steps):
        part = slice(step * step_rows * keys, (step + 1) * step_rows * keys)
        back(step, flat[part], hidden[part])
    for step in range(steps):
        copy_out(step).wait()
    single_copy.wait()


def token_kernel(token_ref):
    token_ref[...] = jnp.zeros(token_ref.shape, token_ref.dtype)


def local_call(
    kernel, operands, outs, name, scratch=(), hbm_out=False, grant=24 * 2**20, flops=0
):
    out_space = pltpu.HBM if hbm_out else pltpu.VMEM
    out_specs = [pl.BlockSpec(memory_space=out_space) for _ in outs]
    if len(outs) == 1:
        outs, out_specs = outs[0], out_specs[0]
    return pl.pallas_call(
        kernel,
        out_shape=outs,
        in_specs=[pl.BlockSpec(memory_space=pltpu.VMEM) for _ in operands],
        out_specs=out_specs,
        scratch_shapes=list(scratch),
        compiler_params=pltpu.CompilerParams(vmem_limit_bytes=grant),
        cost_estimate=pl.CostEstimate(flops=flops, bytes_accessed=2**18, transcendentals=0),
        name=name,
    )(*operands)


def exchange(array, axis, count):
    return [
        lax.ppermute(array, axis, [(i, i ^ k) for i in range(count)]) for k in range(1, count)
    ]


def headwise_body(
    single,
    pair,
    chain,
    live,
    step_index,
    time_scale,
    time_shift,
    w_query,
    w_key,
    w_value,
    w_gate,
    w_out,
    pair_gain,
    bias_weight,
    chain_bias,
    outer_gain,
    w_left,
    w_right,
    w_outer,
    outer_bias,
    trans_gain,
    w_in,
    w_down,
):
    bf16, f32 = jnp.bfloat16, jnp.float32
    rows, width = single.shape
    keys, channels = pair.shape[1:]
    half = rows // 2
    head_count = chain_bias.shape[1]
    count = lax.axis_size("col")
    heads_here = head_count // count
    factors = w_left.shape[1]
    col_place = lax.axis_index("col")
    shape = jax.ShapeDtypeStruct
    token = local_call(token_kernel, (), [shape((8, 128), f32)], "token", flops=10**10)
    packed, aux = local_call(
        pack_kernel,
        (
            token,
            step_index[None],
            time_scale.T,
            time_shift.T,
            outer_gain[None],
            w_left.T,
            w_right.T,
            chain[None],
            live[None],
            bias_weight.T,
            chain_bias,
            outer_bias[None],
            trans_gain[None],
            pair_gain[None],
            single,
        ),
        [shape((rows + 16, width), bf16), shape((AUX_ROWS, channels), f32)],
        "pack",
        flops=10**10,
    )
    blocks = [packed] + exchange(packed, "col", count)

    bias = local_call(
        bias_kernel,
        (aux, pair),
        [shape((count, heads_here, half, 2 * keys), f32)],
        "pair_bias",
        flops=10**10,
    )
    pieces = [lax.dynamic_index_in_dim(bias, col_place ^ k, 0, keepdims=False) for k in range(count)]
    biases = pieces[:1] + [
        lax.ppermute(pieces[k], "col", [(i, i ^ k) for i in range(count)]) for k in range(2, count)
    ]

    query, kv, gate = local_call(
        project_kernel,
        (*blocks, w_query.T, w_key.T, w_value.T, w_gate.T),
        [shape((rows, width), bf16), shape((rows, 2 * width), bf16), shape((rows, width), bf16)],
        "project",
        scratch=(pltpu.VMEM((count, rows, width), bf16),),
        flops=10**8,
    )
    kvs = [kv] + exchange(kv, "row", count)
    near, kv = lax.optimization_barrier((pieces[1], kv))
    biases.insert(1, lax.ppermute(near, "col", [(i, i ^ 1) for i in range(count)]))
    gated = local_call(
        attend_kernel,
        (query, gate, *kvs, *biases),
        [shape((rows * width // 128, 128), bf16)],
        "attend",
        scratch=(
            pltpu.VMEM((count * rows, 2 * width), bf16),
            pltpu.VMEM((count, heads_here, half, 2 * keys), f32),
        ),
        flops=10**8,
    )
    gateds = [gated] + exchange(gated, "col", count)
    result, message = local_call(
        output_kernel,
        (single, outer_gain[None], w_out.T, w_left.T, w_right.T, *gateds),
        [shape((rows, width), bf16), shape((count * count, half + 8, 2 * keys), bf16)],
        "project_out",
        scratch=(pltpu.VMEM((count, rows * width // 128, 128), bf16),),
        flops=10**7,
    )
    outer_flat = w_outer.reshape(factors, factors * channels)
    message, outer_flat = lax.optimization_barrier((message, outer_flat))
    message = lax.all_to_all(message, ("row", "col"), 0, 0)

    steps = 4
    single_out, pair_out = local_call(
        update_kernel,
        (
            result,
            message,
            pair,
            aux,
            outer_flat,
            w_in,
            w_down,
            *blocks,
        ),
        [shape((rows, width), bf16), shape(pair.shape, bf16)],
        "pair_update",
        scratch=(
            pltpu.VMEM(pair.shape, bf16),
            pltpu.VMEM((rows, 2 * factors + 16, channels), bf16),
            pltpu.VMEM((keys, 2 * factors + 16), bf16),
            pltpu.VMEM((w_in.shape[0], w_down.shape[0]), bf16),
            pltpu.SemaphoreType.DMA,
            pltpu.SemaphoreType.DMA((steps,)),
        ),
        hbm_out=True,
        flops=2 * 10**9,
    )
    return (single_out, pair_out)


def pick_body(mesh):
    rows, cols = mesh.shape["row"], mesh.shape["col"]

    def chosen(*arrays):
        single, pair, chain_bias = arrays[0], arrays[1], arrays[14]
        fits = (
            rows == cols
            and cols & (cols - 1) == 0
            and chain_bias.shape[1] % cols == 0
            and single.shape[0] == pair.shape[1] == 64
            and 4 * arrays[16].shape[1] == pair.shape[2]
            and chain_bias.shape[1] <= AUX_ROWS - AUX_WEIGHT
            and pair.shape[2] == 128
            and cols * single.shape[1] == 64 * chain_bias.shape[1]
        )
        return headwise_body(*arrays) if fits else body(*arrays)

    return chosen


def solution(mesh):
    in_specs = (
        P(("groups", "row"), "col"),
        P(("groups", "row"), "col", None),
        P("groups"),
        P("groups"),
        P("groups"),
        P(None, "col"),
        P(None, "col"),
        P(None, "col"),
        P(None, "col"),
        P(None, "col"),
        P(None, "col"),
        P(None, "col"),
        P(),
        P(),
        P(),
        P("col"),
        P("col", None),
        P("col", None),
        P(),
        P(),
        P(),
        P(),
        P(),
    )
    out_specs = (P(("groups", "row"), "col"), P(("groups", "row"), "col", None))
    return jax.shard_map(
        pick_body(mesh), mesh=mesh, in_specs=in_specs, out_specs=out_specs, check_vma=False)
```
